768 devices in a mesh: gz: 96 (over z, x, core), gy: 8 (over y).
Axes of the slice: x: 4, y: 8, z: 12, core: 2. Of those that a mesh axis runs over, the one named last changes fastest.
Arguments:
- right_side: float32 [768, 64, 256], P('gz', 'gy'), may hold values from -10 to 10, as said below
Outputs:
- solution_field: float32 [768, 64, 256], P('gz', 'gy')
- residual: float32 [768, 64, 256], P('gz', 'gy')
The draws below stay inside these ranges and needn't reach their ends.
Inputs may be any that keep to these rules, and one draw needn't show every extreme that they name: `right_side`: a right-hand side.
All inputs are finite; a program needn't handle non-finite values.
Results may differ from the reference program's by a relative error of at most 0.00015.
Values sent between devices are 32-bit elements; how exact they have to be, the bound alone decides.
A program may use at most 32 MiB of HBM per device.

```python
import math
import jax
import jax.numpy as jnp

NX = 256
LEVELS = 3
NZ = 768
NY = 64


def draw_right_side(key, part):
    keys = jax.random.split(jax.random.fold_in(key, 11), 3)
    z_pos = jnp.arange(NZ, dtype=jnp.float32) / (NZ - 1)
    z_cell = jnp.arange(NZ, dtype=jnp.float32)[:, None, None]
    y_cell = jnp.arange(NY, dtype=jnp.float32)[None, :, None]
    x_cell = jnp.arange(NX, dtype=jnp.float32)[None, None, :]
    freqs = jax.random.uniform(keys[1], (4, 3), jnp.float32, 0.025, 0.1)
    phases = jax.random.uniform(keys[2], (4, 3), jnp.float32, 0.0, 2.0 * math.pi)
    smooth = jnp.zeros((NZ, NY, NX), jnp.float32)
    for term in range(4):
        smooth = smooth + 0.5 * (jnp.cos(2.0 * math.pi * freqs[term, 0] * z_cell + phases[term, 0]) * jnp.cos(2.0 * math.pi * freqs[term, 1] * y_cell + phases[term, 1]) * jnp.cos(2.0 * math.pi * freqs[term, 2] * x_cell + phases[term, 2]))
    smooth = jnp.clip(smooth, -2.0, 2.0)
    share = (0.15 + 0.85 * z_pos)[:, None, None]
    amplitude = jnp.exp(math.log(2.0) * z_pos)[:, None, None]
    noise = jnp.clip(jax.random.normal(keys[0], (NZ, NY, NX), jnp.float32), -3.5, 3.5)
    values = amplitude * (share * noise + (1.0 - share) * smooth)
    return jnp.clip(values, -10.0, 10.0).astype(jnp.float32)


def setup_inputs(seed: int = 0) -> dict:
    seeds = jax.random.split(jax.random.key(seed), 2)
    right_side = draw_right_side(jax.random.fold_in(seeds[1], 71), 0)
    return dict(right_side=right_side)


sweep_order = [((0, 0), (0, 1)), ((0, 1), (0, 1)), ((1, 0), (0, 1)), ((1, 1), (0, 1)),
               ((1, 1), (1, 0)), ((1, 0), (1, 0)), ((0, 1), (1, 0)), ((0, 0), (1, 0))]


def x_side(field):
    width = [(0, 0)] * (field.ndim - 1)
    upper = jnp.pad(field[..., 1:], width + [(0, 1)])
    lower = jnp.pad(field[..., :-1], width + [(1, 0)])
    return upper + lower


def operate(padded):
    z_cells = padded.shape[0] - 2
    y_cells = padded.shape[1] - 2
    boxed = jnp.zeros((z_cells, y_cells, padded.shape[2]), jnp.float32)
    for z_step in range(3):
        for y_step in range(3):
            boxed = boxed + padded[z_step:z_step + z_cells, y_step:y_step + y_cells, :]
    boxed = boxed + x_side(boxed)
    return 27.0 * padded[1:-1, 1:-1, :] - boxed


def group_update(padded, rhs, z_par, y_par, x_order):
    z_cells = padded.shape[0] - 2
    y_cells = padded.shape[1] - 2
    outer = None
    for z_step in (-1, 0, 1):
        for y_step in (-1, 0, 1):
            if z_step == 0 and y_step == 0:
                continue
            row = padded[1 + z_par + z_step:z_cells + z_par + z_step:2, 1 + y_par + y_step:y_cells + y_par + y_step:2, :]
            outer = row if outer is None else outer + row
    center = padded[1 + z_par:z_cells + z_par:2, 1 + y_par:y_cells + y_par:2, :]
    total = outer + x_side(outer) + rhs[z_par::2, y_par::2, :]
    parity = jnp.arange(padded.shape[2], dtype=jnp.int32) % 2
    for x_par in x_order:
        center = jnp.where(parity == x_par, (total + x_side(center)) / 26.0, center)
    return padded.at[1 + z_par:z_cells + z_par:2, 1 + y_par:y_cells + y_par:2, :].set(center)


def pad_zero(field):
    return jnp.pad(field, ((1, 1), (1, 1), (0, 0)))


def symmetric_sweeps(rhs, start):
    padded = pad_zero(start)
    for group, x_order in sweep_order:
        padded = group_update(padded, rhs, group[0], group[1], x_order)
    return padded[1:-1, 1:-1, :]


def vcycle(rhs, level):
    zeros = jnp.zeros_like(rhs)
    if level == LEVELS - 1:
        return symmetric_sweeps(rhs, zeros)
    first = symmetric_sweeps(rhs, zeros)
    defect = rhs - operate(pad_zero(first))
    coarse = vcycle(defect[::2, ::2, ::2], level + 1)
    return symmetric_sweeps(rhs, first.at[::2, ::2, ::2].add(coarse))


def reference(right_side):
    precond = vcycle(right_side, 0)
    image = operate(pad_zero(precond))
    alpha = jnp.sum(right_side * precond) / jnp.sum(precond * image)
    return alpha * precond, right_side - alpha * image
```

```python
import functools

import jax
import jax.numpy as jnp
from jax import lax
from jax.experimental import pallas as pl
from jax.experimental.pallas import tpu as pltpu
from jax.sharding import PartitionSpec as P

MESH = pl.DeviceIdType.MESH
F32 = jnp.float32
INV = 1.0 / 26.0
NX_CHIPS = 4
CORES = 2

SWEEP = [
    ((0, 0), (0, 1)),
    ((0, 1), (0, 1)),
    ((1, 0), (0, 1)),
    ((1, 1), (0, 1, 0)),
    ((1, 0), (1, 0)),
    ((0, 1), (1, 0)),
    ((0, 0), (1, 0)),
]
PRE_ROWS = [(1, 11), (1, 10), (2, 10), (2, 9), (3, 9), (3, 8), (4, 8)]
POST_ROWS = [(1, 12), (1, 11), (2, 11), (2, 10), (3, 10), (3, 9), (4, 9)]


def lanes(shape):
    return lax.broadcasted_iota(jnp.int32, shape, len(shape) - 1)


def sublanes(shape):
    return lax.broadcasted_iota(jnp.int32, shape, len(shape) - 2)


def from_left(u, step=1):
    return jnp.where(lanes(u.shape) >= step, pltpu.roll(u, step, u.ndim - 1), 0.0)


def from_right(u, step=1):
    return jnp.where(lanes(u.shape) < 128 - step, pltpu.roll(u, 128 - step, u.ndim - 1), 0.0)


def both_sides(u, step=1):
    return from_left(u, step) + from_right(u, step)


def down(u):
    return pltpu.roll(u, 1, u.ndim - 2)


def up(u):
    return pltpu.roll(u, 7, u.ndim - 2)


def remote(src, dst, send, recv, where):
    copy = pltpu.make_async_remote_copy(
        src_ref=src, dst_ref=dst, send_sem=send, recv_sem=recv, device_id=where, device_id_type=MESH
    )
    return copy


def kernel(
    ngz, ngy, r_ref, sol_ref, res_ref,
    rw, rd, f0, v0, p0, mk, own, fw, dcb, dall, f1, v1, p1, f2, v2, vc, stage, prec, imag, sb, ar1, ar2,
    rs, rr, fs, fr, cs, cr, s1, r1, s2, r2,
):
    gz = lax.axis_index("gz")
    gy = lax.axis_index("gy")
    nz = ngz // (NX_CHIPS * CORES)
    core = lax.rem(gz, CORES)
    chip_x = lax.rem(gz // CORES, NX_CHIPS)
    chip_z = gz // (CORES * NX_CHIPS)

    def at(dz, dy):
        return (lax.rem(gz + dz + ngz, ngz), lax.rem(gy + dy + ngy, ngy))

    def along_z(dc, dz):
        z = lax.rem(chip_z + dz + nz, nz)
        return ((z * NX_CHIPS + chip_x) * CORES + lax.rem(core + dc, CORES), gy)

    def along_xy(dx, dy):
        x = lax.rem(chip_x + dx + NX_CHIPS, NX_CHIPS)
        return ((chip_z * NX_CHIPS + x) * CORES + core, lax.rem(gy + dy + ngy, ngy))

    coarse_sends = [
        (slot, dz, dy)
        for dy in range(ngy)
        for slot, dz in ((2, 0), (1, 1), (3, -1), (0, 2))
        if not (dz == 0 and dy == 0)
    ]
    first_group = [(c, z) for z in range(nz) for c in range(CORES) if (c, z) != (0, 0)]
    second_group = [(x, y) for y in range(ngy) for x in range(NX_CHIPS) if (x, y) != (0, 0)]
    halo = [(dz, dy) for dz in (0, 1, -1) for dy in (0, 1, -1) if (dz, dy) != (0, 0)]

    barrier = pltpu.get_barrier_semaphore()
    for slot, dz, dy in coarse_sends:
        pl.semaphore_signal(barrier, inc=1, device_id=at(-dz, -dy), device_id_type=MESH)
    for c, z in first_group:
        pl.semaphore_signal(barrier, inc=1, device_id=along_z(-c + CORES, -z), device_id_type=MESH)
    for x, y in second_group:
        pl.semaphore_signal(barrier, inc=1, device_id=along_xy(-x, -y), device_id_type=MESH)

    for yb in range(3):
        for zi in (0, 14, 15):
            rw[yb, zi] = jnp.zeros((8, 256), F32)
        fw[yb, :, 120:128, :] = jnp.zeros((2, 8, 128), F32)
    fw[1, :, 24:88, :] = jnp.zeros((2, 64, 128), F32)
    rw[1, 3:11] = r_ref[...]
    dall[:, 0:8, :] = jnp.zeros((ngy, 8, 128), F32)
    v0[...] = jnp.zeros(v0.shape, F32)
    p0[...] = jnp.zeros(p0.shape, F32)
    v1[...] = jnp.zeros(v1.shape, F32)
    p1[...] = jnp.zeros(p1.shape, F32)
    v2[...] = jnp.zeros(v2.shape, F32)

    sub = sublanes((8, 128))
    for zp in range(2):
        z = gz * 8 + 2 * sub - (2 + zp)
        z_in = ((z >= 0) & (z < ngz * 8)).astype(F32)
        low = jnp.where(gy > 0, 1.0, 0.0).astype(F32)
        high = jnp.where(gy < ngy - 1, 1.0, 0.0).astype(F32)
        mk[zp, 0:4] = jnp.broadcast_to(z_in * low, (4, 8, 128))
        mk[zp, 4:8] = jnp.broadcast_to(z_in, (4, 8, 128))
        mk[zp, 8:12] = jnp.broadcast_to(z_in * high, (4, 8, 128))

    def own_rows(zp, shape):
        s = sublanes(shape)
        return (s >= 1 + zp) & (s < 5 + zp)

    pl.semaphore_wait(barrier, len(coarse_sends) + len(first_group) + len(second_group))

    rhs_rows = {0: (0, 8, 3), 1: (6, 2, 1), -1: (0, 3, 11)}
    rhs_copies = []
    for k, (dz, dy) in enumerate(halo):
        z_from, count, z_to = rhs_rows[dz]
        copy = remote(
            r_ref.at[pl.ds(z_from, count)], rw.at[1 - dy, pl.ds(z_to, count)], rs.at[k], rr.at[k], at(dz, dy)
        )
        copy.start()
        rhs_copies.append(copy)

    row = lax.broadcasted_iota(jnp.int32, (256, 256), 0)
    col = lax.broadcasted_iota(jnp.int32, (256, 256), 1)
    split = (row == jnp.where(col < 128, 2 * col, 2 * col - 255)).astype(F32)
    merge = (col == jnp.where(row < 128, 2 * row, 2 * row - 255)).astype(F32)

    def permuted(block, matrix):
        return lax.dot_general(
            block, matrix, (((1,), (0,)), ((), ())), precision=lax.Precision.HIGHEST, preferred_element_type=F32
        )

    for copy in rhs_copies:
        copy.wait_recv()
    for yb in range(3):
        both = permuted(rw[yb].reshape(128, 256), split)
        rd[yb, 0] = both[:, :128]
        rd[yb, 1] = both[:, 128:]

    def window(zp, yp, i):
        return i // 4, pl.ds(8 * (1 - zp) + 2 * (i % 4) + yp, 8, stride=16)

    for zp in range(2):
        for yp in range(2):
            for xp in range(2):
                for i in range(12):
                    yb, rows = window(zp, yp, i)
                    f0[zp, yp, xp, i] = rd[yb, xp, rows, :]

    def pair0(zp, c):
        return c + (down(c) if zp == 0 else up(c))

    def outer0(zp, yp, lo, hi):
        a = -1 if yp == 0 else 0
        sums = []
        for xp in range(2):
            s = v0[zp, 1 - yp, xp, lo + a : hi + a] + v0[zp, 1 - yp, xp, lo + a + 1 : hi + a + 1]
            q = p0[1 - zp, 1 - yp, xp, lo + a : hi + a] + p0[1 - zp, 1 - yp, xp, lo + a + 1 : hi + a + 1]
            sums.append(s + q + p0[1 - zp, yp, xp, lo:hi])
        return sums

    def around0(s, c, xp):
        other = s[1 - xp] + c[1 - xp]
        return s[xp] + (other + (from_left(other) if xp == 0 else from_right(other)))

    def phase0(group, order, lo, hi):
        zp, yp = group
        s = outer0(zp, yp, lo, hi)
        c = [v0[zp, yp, 0, lo:hi], v0[zp, yp, 1, lo:hi]]
        scale = mk[zp, lo:hi] * INV
        for xp in order:
            c[xp] = (around0(s, c, xp) + f0[zp, yp, xp, lo:hi]) * scale
        for xp in range(2):
            v0[zp, yp, xp, lo:hi] = c[xp]
            p0[zp, yp, xp, lo:hi] = pair0(zp, c[xp])

    for (group, order), (lo, hi) in zip(SWEEP, PRE_ROWS):
        phase0(group, order, lo, hi)

    for zp in range(2):
        for yp in range(2):
            for xp in range(2):
                for i in range(4, 8):
                    own[xp, window(zp, yp, i)[1], :] = v0[zp, yp, xp, i]
    field_rows = {0: (3, 8, 3), 1: (8, 3, 0), -1: (3, 4, 11)}
    field_copies = []
    s = outer0(0, 0, 4, 8)
    c = [v0[0, 0, 0, 4:8], v0[0, 0, 1, 4:8]]
    defect = up(f0[0, 0, 0, 4:8] - (26.0 * c[0] - around0(s, c, 0)))
    for i in range(4):
        dcb[pl.ds(i, 8, stride=4), :] = defect[i]
    for k, (dz, dy) in enumerate(halo):
        z_from, count, z_to = field_rows[dz]
        copy = remote(
            own.at[:, pl.ds(8 * z_from, 8 * count), :],
            fw.at[1 - dy, :, pl.ds(8 * z_to, 8 * count), :],
            fs.at[k], fr.at[k], at(dz, dy),
        )
        copy.start()
        field_copies.append(copy)
    coarse_copies = []
    for k, (slot, dz, dy) in enumerate(coarse_sends):
        first, count = (8, 8) if slot == 0 else (0, 16)
        copy = remote(
            dcb.at[pl.ds(first, count), :], dall.at[gy, pl.ds(16 * slot + first, count), :],
            cs.at[k], cr.at[k], at(dz, dy),
        )
        copy.start()
        coarse_copies.append(copy)
    dall[gy, 32:48, :] = dcb[0:16, :]

    for copy in field_copies:
        copy.wait_recv()
    for zp in range(2):
        for yp in range(2):
            for xp in range(2):
                for i in range(12):
                    yb, rows = window(zp, yp, i)
                    value = fw[yb, xp, rows, :] * mk[zp, i]
                    if yb == 1:
                        value = jnp.where(own_rows(zp, (8, 128)), v0[zp, yp, xp, i], value)
                    v0[zp, yp, xp, i] = value
                    if zp == 1:
                        p0[zp, yp, xp, i] = pair0(zp, value)

    for copy in coarse_copies:
        copy.wait_recv()

    n1 = 2 * ngy
    for zp in range(2):
        for yp in range(2):
            for i in range(n1):
                f1[zp, yp, i] = dall[i // 2, pl.ds(2 * (i % 2) + yp + 4 * zp, 8, stride=8), :]

    scale1 = []
    for zp in range(2):
        z = gz * 4 + 2 * sub - (8 - zp)
        scale1.append(jnp.where((z >= 0) & (z < ngz * 4), INV, 0.0).astype(F32)[None])

    def pair1(zp, c):
        return c + (up(c) if zp == 0 else down(c))

    def outer1(zp, yp):
        a = 0 if yp == 0 else 1
        s = v1[zp, 1 - yp, a : a + n1] + v1[zp, 1 - yp, a + 1 : a + 1 + n1]
        q = p1[1 - zp, 1 - yp, a : a + n1] + p1[1 - zp, 1 - yp, a + 1 : a + 1 + n1]
        return s + q + p1[1 - zp, yp, 1 : 1 + n1]

    def phase1(group, order):
        zp, yp = group
        s = outer1(zp, yp)
        c = v1[zp, yp, 1 : 1 + n1]
        base = s + f1[zp, yp]
        parity = lax.rem(lanes(c.shape), 2)
        for xp in order:
            c = jnp.where(parity == xp, (base + both_sides(s + c)) * scale1[zp], c)
        v1[zp, yp, 1 : 1 + n1] = c
        p1[zp, yp, 1 : 1 + n1] = pair1(zp, c)

    for group, order in SWEEP:
        phase1(group, order)

    n2 = ngy
    s = outer1(0, 0)
    c = v1[0, 0, 1 : 1 + n1]
    even = lax.rem(lanes(c.shape), 2) == 0
    defect = jnp.where(even, f1[0, 0] - (26.0 * c - (s + both_sides(s + c))), 0.0)
    for i in range(n1):
        f2[i % 2, i // 2] = defect[i]
    z = gz * 2 + sub - 4
    scale2 = jnp.where((z >= 0) & (z < ngz * 2), INV, 0.0).astype(F32)[None]

    for group, order in SWEEP:
        zp, yp = group
        a = 0 if yp == 0 else 1
        c = v2[yp, 1 : 1 + n2]
        side = v2[1 - yp, a : a + n2] + v2[1 - yp, a + 1 : a + 1 + n2]
        column = side + c
        s = side + (down(column) + up(column))
        base = s + f2[yp]
        layer = lax.rem(sublanes(c.shape), 2) == zp
        place = lax.rem(lanes(c.shape), 4)
        for xp in order:
            c = jnp.where(layer & (place == 2 * xp), (base + both_sides(s + c, 2)) * scale2, c)
        v2[yp, 1 : 1 + n2] = c

    held = sublanes((8, 128))
    mine = (held >= 4) & (held < 6)
    for i in range(n1):
        value = v1[0, 0, 1 + i] + jnp.where(mine, v2[i % 2, 1 + i // 2], 0.0)
        v1[0, 0, 1 + i] = value
        p1[0, 0, 1 + i] = pair1(0, value)
    for group, order in SWEEP:
        phase1(group, order)

    for i in range(4):
        for zp in range(2):
            vc[i, pl.ds(zp, 8, stride=2), :] = v1[zp, i % 2, 1 + 2 * gy + i // 2]
    for i in range(4):
        v0[0, 0, 0, 4 + i] += jnp.where(own_rows(0, (8, 128)), vc[i, 7:15, :], 0.0)

    for (group, order), (lo, hi) in zip(SWEEP, POST_ROWS):
        phase0(group, order, lo, hi)

    numer = jnp.zeros((8, 128), F32)
    denom = jnp.zeros((8, 128), F32)
    images = {}
    for zp in range(2):
        for yp in range(2):
            s = outer0(zp, yp, 4, 8)
            c = [v0[zp, yp, 0, 4:8], v0[zp, yp, 1, 4:8]]
            mine = own_rows(zp, (8, 128))
            top, bottom = 0.0, 0.0
            for xp in range(2):
                image = 26.0 * c[xp] - around0(s, c, xp)
                images[zp, yp, xp] = image
                top = top + jnp.sum(c[xp] * f0[zp, yp, xp, 4:8], axis=0)
                bottom = bottom + jnp.sum(c[xp] * image, axis=0)
            numer = numer + jnp.where(mine, top, 0.0)
            denom = denom + jnp.where(mine, bottom, 0.0)
    lower = lanes((8, 128)) < 64
    both = jnp.where(lower, numer + pltpu.roll(numer, 64, 1), denom + pltpu.roll(denom, 64, 1))
    part = jnp.sum(both, axis=0, keepdims=True)
    sb[0] = part
    first_copies = []
    for k, (c, z) in enumerate(first_group):
        copy = remote(sb.at[0], ar1.at[k], s1.at[k], r1.at[k], along_z(c, z))
        copy.start()
        first_copies.append(copy)

    for zp in range(2):
        for yp in range(2):
            for xp in range(2):
                for i in range(4):
                    rows = window(zp, yp, 4 + i)[1]
                    stage[0, xp, rows, :] = v0[zp, yp, xp, 4 + i]
                    stage[1, xp, rows, :] = images[zp, yp, xp][i]
    for t, target in enumerate((prec, imag)):
        block = jnp.concatenate([stage[t, 0, 24:88, :], stage[t, 1, 24:88, :]], axis=1)
        target[...] = permuted(block, merge).reshape(8, 8, 256)

    for copy in first_copies:
        copy.wait_recv()
    part = part + jnp.sum(ar1[...], axis=0)
    sb[1] = part
    second_copies = []
    for k, (x, y) in enumerate(second_group):
        copy = remote(sb.at[1], ar2.at[k], s2.at[k], r2.at[k], along_xy(x, y))
        copy.start()
        second_copies.append(copy)
    for copy in second_copies:
        copy.wait_recv()
    part = part + jnp.sum(ar2[...], axis=0)
    left = lanes((1, 128)) < 64
    total_n = jnp.sum(jnp.where(left, part, 0.0), axis=1, keepdims=True)
    total_d = jnp.sum(jnp.where(left, 0.0, part), axis=1, keepdims=True)
    alpha = (total_n / total_d)[:, :, None]
    sol_ref[...] = alpha * prec[...]
    res_ref[...] = r_ref[...] - alpha * imag[...]

    for copy in rhs_copies + field_copies + coarse_copies + first_copies + second_copies:
        copy.wait_send()


def solution(mesh):
    ngz, ngy = mesh.shape["gz"], mesh.shape["gy"]
    nz = ngz // (NX_CHIPS * CORES)
    coarse = 4 * ngy - 1
    one = nz * CORES - 1
    two = NX_CHIPS * ngy - 1

    def body(right_side):
        out = jax.ShapeDtypeStruct(right_side.shape, F32)
        vm = pltpu.VMEM
        dma = pltpu.SemaphoreType.DMA
        return pl.pallas_call(
            functools.partial(kernel, ngz, ngy),
            name="cg_iteration",
            out_shape=(out, out),
            in_specs=[pl.BlockSpec(memory_space=pltpu.VMEM)],
            out_specs=(pl.BlockSpec(memory_space=pltpu.VMEM), pl.BlockSpec(memory_space=pltpu.VMEM)),
            scratch_shapes=[
                vm((3, 16, 8, 256), F32),
                vm((3, 2, 128, 128), F32),
                vm((2, 2, 2, 12, 8, 128), F32),
                vm((2, 2, 2, 12, 8, 128), F32),
                vm((2, 2, 2, 12, 8, 128), F32),
                vm((2, 12, 8, 128), F32),
                vm((2, 128, 128), F32),
                vm((3, 2, 128, 128), F32),
                vm((32, 128), F32),
                vm((ngy, 64, 128), F32),
                vm((2, 2, 2 * ngy, 8, 128), F32),
                vm((2, 2, 2 * ngy + 2, 8, 128), F32),
                vm((2, 2, 2 * ngy + 2, 8, 128), F32),
                vm((2, ngy, 8, 128), F32),
                vm((2, ngy + 2, 8, 128), F32),
                vm((4, 16, 128), F32),
                vm((2, 2, 128, 128), F32),
                vm((8, 8, 256), F32),
                vm((8, 8, 256), F32),
                vm((2, 1, 128), F32),
                vm((one, 1, 128), F32),
                vm((two, 1, 128), F32),
                dma((8,)), dma((8,)), dma((8,)), dma((8,)), dma((coarse,)), dma((coarse,)),
                dma((one,)), dma((one,)), dma((two,)), dma((two,)),
            ],
            compiler_params=pltpu.CompilerParams(collective_id=0, has_side_effects=True),
        )(right_side)

    return jax.shard_map(
        body,
        mesh=mesh,
        in_specs=(P("gz", "gy", None),),
        out_specs=(P("gz", "gy", None), P("gz", "gy", None)),
        check_vma=False,
    )
```

```python
import functools

import jax
import jax.numpy as jnp
from jax import lax
from jax.experimental import pallas as pl
from jax.experimental.pallas import tpu as pltpu
from jax.sharding import PartitionSpec as P

MESH = pl.DeviceIdType.MESH
F32 = jnp.float32
INV = 1.0 / 26.0
NX_CHIPS = 4
CORES = 2

SWEEP = [
    ((0, 0), (0, 1)),
    ((0, 1), (0, 1)),
    ((1, 0), (0, 1)),
    ((1, 1), (0, 1, 0)),
    ((1, 0), (1, 0)),
    ((0, 1), (1, 0)),
    ((0, 0), (1, 0)),
]
PRE_ROWS = [(1, 11), (1, 10), (2, 10), (2, 9), (3, 9), (3, 8), (4, 8)]
POST_ROWS = [(1, 12), (1, 11), (2, 11), (2, 10), (3, 10), (3, 9), (4, 9)]


def lanes(shape):
    return lax.broadcasted_iota(jnp.int32, shape, len(shape) - 1)


def sublanes(shape):
    return lax.broadcasted_iota(jnp.int32, shape, len(shape) - 2)


def from_left(u, step=1):
    return jnp.where(lanes(u.shape) >= step, pltpu.roll(u, step, u.ndim - 1), 0.0)


def from_right(u, step=1):
    return jnp.where(lanes(u.shape) < 128 - step, pltpu.roll(u, 128 - step, u.ndim - 1), 0.0)


def both_sides(u, step=1):
    return from_left(u, step) + from_right(u, step)


def down(u):
    return pltpu.roll(u, 1, u.ndim - 2)


def up(u):
    return pltpu.roll(u, 7, u.ndim - 2)


def remote(src, dst, send, recv, where):
    copy = pltpu.make_async_remote_copy(
        src_ref=src, dst_ref=dst, send_sem=send, recv_sem=recv, device_id=where, device_id_type=MESH
    )
    return copy


def kernel(
    ngz, ngy, r_hbm, prec_hbm, imag_hbm, alpha_ref,
    rin, ownr, rd, f0, v0, p0, mk, own, fw, dcb, dall, f1, v1, p1, f2, v2, vc, stage, prec, imag, sb, ar1, ar2,
    io, rs, rr, fs, fr, cs, cr, s1, r1, s2, r2,
):
    gz = lax.axis_index("gz")
    gy = lax.axis_index("gy")
    nz = ngz // (NX_CHIPS * CORES)
    core = lax.rem(gz, CORES)
    chip_x = lax.rem(gz // CORES, NX_CHIPS)
    chip_z = gz // (CORES * NX_CHIPS)

    def at(dz, dy):
        return (lax.rem(gz + dz % ngz, ngz), lax.rem(gy + dy % ngy, ngy))

    def along_z(dc, dz):
        z = lax.rem(chip_z + dz % nz, nz)
        return ((z * NX_CHIPS + chip_x) * CORES + lax.rem(core + dc % CORES, CORES), gy)

    def along_xy(dx, dy):
        x = lax.rem(chip_x + dx % NX_CHIPS, NX_CHIPS)
        return ((chip_z * NX_CHIPS + x) * CORES + core, lax.rem(gy + dy % ngy, ngy))

    coarse_sends = [
        (slot, dz, dy)
        for dy in sorted(range(ngy), key=lambda d: -min(d, ngy - d))
        for slot, dz in ((2, 0), (1, 1), (3, -1), (0, 2))
        if not (dz == 0 and dy == 0)
    ]
    first_group = [(c, z) for z in range(nz) for c in range(CORES) if (c, z) != (0, 0)]
    first_group.sort(key=lambda g: -min(g[1], nz - g[1]))
    second_group = [(x, y) for y in range(ngy) for x in range(NX_CHIPS) if (x, y) != (0, 0)]
    second_group.sort(key=lambda g: -min(g[1], ngy - g[1]) - min(g[0], NX_CHIPS - g[0]))
    halo = [(dz, dy) for dz in (0, 1, -1) for dy in (0, 1, -1) if (dz, dy) != (0, 0)]

    load = pltpu.make_async_copy(r_hbm, rin, io.at[0])
    load.start()

    barrier = pltpu.get_barrier_semaphore()
    for c, z in first_group:
        pl.semaphore_signal(barrier, inc=1, device_id=along_z(-c, -z), device_id_type=MESH)
    for x, y in second_group:
        pl.semaphore_signal(barrier, inc=1, device_id=along_xy(-x, -y), device_id_type=MESH)
    for slot, dz, dy in coarse_sends:
        pl.semaphore_signal(barrier, inc=1, device_id=at(-dz, -dy), device_id_type=MESH)

    row = lax.broadcasted_iota(jnp.int32, (256, 256), 0)
    col = lax.broadcasted_iota(jnp.int32, (256, 256), 1)
    split = (row == jnp.where(col < 128, 2 * col, 2 * col - 255)).astype(F32)
    merge = (col == jnp.where(row < 128, 2 * row, 2 * row - 255)).astype(F32)

    def permuted(block, matrix):
        return lax.dot_general(
            block, matrix, (((1,), (0,)), ((), ())), precision=lax.Precision.HIGHEST, preferred_element_type=F32
        )

    load.wait()
    both = permuted(rin[...].reshape(64, 256), split)
    for xp in range(2):
        part = both[:, 128 * xp : 128 * xp + 128]
        ownr[xp] = part
        rd[1, xp, 24:88, :] = part

    for yb in range(3):
        rd[yb, :, 0:8, :] = jnp.zeros((2, 8, 128), F32)
        rd[yb, :, 112:128, :] = jnp.zeros((2, 16, 128), F32)
        fw[yb, :, 120:128, :] = jnp.zeros((2, 8, 128), F32)
    fw[1, :, 24:88, :] = jnp.zeros((2, 64, 128), F32)
    dall[:, 0:8, :] = jnp.zeros((ngy, 8, 128), F32)
    v0[...] = jnp.zeros(v0.shape, F32)
    p0[...] = jnp.zeros(p0.shape, F32)
    v1[...] = jnp.zeros(v1.shape, F32)
    p1[...] = jnp.zeros(p1.shape, F32)
    v2[...] = jnp.zeros(v2.shape, F32)

    sub = sublanes((8, 128))
    for zp in range(2):
        z = gz * 8 + 2 * sub - (2 + zp)
        z_in = ((z >= 0) & (z < ngz * 8)).astype(F32)
        low = jnp.where(gy > 0, 1.0, 0.0).astype(F32)
        high = jnp.where(gy < ngy - 1, 1.0, 0.0).astype(F32)
        mk[zp, 0:4] = jnp.broadcast_to(z_in * low, (4, 8, 128))
        mk[zp, 4:8] = jnp.broadcast_to(z_in, (4, 8, 128))
        mk[zp, 8:12] = jnp.broadcast_to(z_in * high, (4, 8, 128))

    def own_rows(zp, shape):
        s = sublanes(shape)
        return (s >= 1 + zp) & (s < 5 + zp)

    pl.semaphore_wait(barrier, len(coarse_sends) + len(first_group) + len(second_group))

    def border(source, target, rows, sends, arrivals):
        copies = []
        for k, (dz, dy) in enumerate(halo):
            z_from, count, z_to = rows[dz]
            copy = remote(
                source.at[:, pl.ds(8 * z_from, 8 * count), :],
                target.at[1 - dy, :, pl.ds(8 * z_to, 8 * count), :],
                sends.at[k], arrivals.at[k], at(dz, dy),
            )
            copy.start()
            copies.append(copy)
        return copies

    rhs_copies = border(ownr, rd, {0: (0, 8, 3), 1: (6, 2, 1), -1: (0, 3, 11)}, rs, rr)
    for copy in rhs_copies:
        copy.wait_recv()

    def window(zp, yp, i):
        return i // 4, pl.ds(8 * (1 - zp) + 2 * (i % 4) + yp, 8, stride=16)

    for zp in range(2):
        for yp in range(2):
            for xp in range(2):
                for i in range(12):
                    yb, rows = window(zp, yp, i)
                    f0[zp, yp, xp, i] = rd[yb, xp, rows, :]

    def pair0(zp, c):
        return c + (down(c) if zp == 0 else up(c))

    def outer0(zp, yp, lo, hi):
        a = -1 if yp == 0 else 0
        sums = []
        for xp in range(2):
            s = v0[zp, 1 - yp, xp, lo + a : hi + a] + v0[zp, 1 - yp, xp, lo + a + 1 : hi + a + 1]
            q = p0[1 - zp, 1 - yp, xp, lo + a : hi + a] + p0[1 - zp, 1 - yp, xp, lo + a + 1 : hi + a + 1]
            sums.append(s + q + p0[1 - zp, yp, xp, lo:hi])
        return sums

    def around0(s, c, xp):
        other = s[1 - xp] + c[1 - xp]
        return s[xp] + (other + (from_left(other) if xp == 0 else from_right(other)))

    def phase0(group, order, lo, hi):
        zp, yp = group
        s = outer0(zp, yp, lo, hi)
        c = [v0[zp, yp, 0, lo:hi], v0[zp, yp, 1, lo:hi]]
        scale = mk[zp, lo:hi] * INV
        for xp in order:
            c[xp] = (around0(s, c, xp) + f0[zp, yp, xp, lo:hi]) * scale
        for xp in range(2):
            v0[zp, yp, xp, lo:hi] = c[xp]
            p0[zp, yp, xp, lo:hi] = pair0(zp, c[xp])

    for (group, order), (lo, hi) in zip(SWEEP, PRE_ROWS):
        phase0(group, order, lo, hi)

    s = outer0(0, 0, 4, 8)
    c = [v0[0, 0, 0, 4:8], v0[0, 0, 1, 4:8]]
    defect = up(f0[0, 0, 0, 4:8] - (26.0 * c[0] - around0(s, c, 0)))
    for i in range(4):
        dcb[pl.ds(i, 8, stride=4), :] = defect[i]
    for zp in range(2):
        for yp in range(2):
            for xp in range(2):
                for i in range(4, 8):
                    own[xp, window(zp, yp, i)[1], :] = v0[zp, yp, xp, i]
    coarse_copies = []
    for k, (slot, dz, dy) in enumerate(coarse_sends):
        first, count = (8, 8) if slot == 0 else (0, 16)
        copy = remote(
            dcb.at[pl.ds(first, count), :], dall.at[gy, pl.ds(16 * slot + first, count), :],
            cs.at[k], cr.at[k], at(dz, dy),
        )
        copy.start()
        coarse_copies.append(copy)
    field_copies = border(own, fw, {0: (3, 8, 3), 1: (8, 3, 0), -1: (3, 4, 11)}, fs, fr)
    dall[gy, 32:48, :] = dcb[0:16, :]

    for copy in coarse_copies:
        copy.wait_recv()

    n1 = 2 * ngy
    for zp in range(2):
        for yp in range(2):
            for i in range(n1):
                f1[zp, yp, i] = dall[i // 2, pl.ds(2 * (i % 2) + yp + 4 * zp, 8, stride=8), :]

    scale1 = []
    for zp in range(2):
        z = gz * 4 + 2 * sub - (8 - zp)
        scale1.append(jnp.where((z >= 0) & (z < ngz * 4), INV, 0.0).astype(F32)[None])

    def pair1(zp, c):
        return c + (up(c) if zp == 0 else down(c))

    def outer1(zp, yp):
        a = 0 if yp == 0 else 1
        s = v1[zp, 1 - yp, a : a + n1] + v1[zp, 1 - yp, a + 1 : a + 1 + n1]
        q = p1[1 - zp, 1 - yp, a : a + n1] + p1[1 - zp, 1 - yp, a + 1 : a + 1 + n1]
        return s + q + p1[1 - zp, yp, 1 : 1 + n1]

    def phase1(group, order):
        zp, yp = group
        s = outer1(zp, yp)
        c = v1[zp, yp, 1 : 1 + n1]
        base = s + f1[zp, yp]
        parity = lax.rem(lanes(c.shape), 2)
        for xp in order:
            c = jnp.where(parity == xp, (base + both_sides(s + c)) * scale1[zp], c)
        v1[zp, yp, 1 : 1 + n1] = c
        p1[zp, yp, 1 : 1 + n1] = pair1(zp, c)

    for group, order in SWEEP:
        phase1(group, order)

    n2 = ngy
    s = outer1(0, 0)
    c = v1[0, 0, 1 : 1 + n1]
    even = lax.rem(lanes(c.shape), 2) == 0
    defect = jnp.where(even, f1[0, 0] - (26.0 * c - (s + both_sides(s + c))), 0.0)
    for i in range(n1):
        f2[i % 2, i // 2] = defect[i]
    z = gz * 2 + sub - 4
    scale2 = jnp.where((z >= 0) & (z < ngz * 2), INV, 0.0).astype(F32)[None]

    for group, order in SWEEP:
        zp, yp = group
        a = 0 if yp == 0 else 1
        c = v2[yp, 1 : 1 + n2]
        side = v2[1 - yp, a : a + n2] + v2[1 - yp, a + 1 : a + 1 + n2]
        column = side + c
        s = side + (down(column) + up(column))
        base = s + f2[yp]
        layer = lax.rem(sublanes(c.shape), 2) == zp
        place = lax.rem(lanes(c.shape), 4)
        for xp in order:
            c = jnp.where(layer & (place == 2 * xp), (base + both_sides(s + c, 2)) * scale2, c)
        v2[yp, 1 : 1 + n2] = c

    held = sublanes((8, 128))
    mine = (held >= 4) & (held < 6)
    for i in range(n1):
        value = v1[0, 0, 1 + i] + jnp.where(mine, v2[i % 2, 1 + i // 2], 0.0)
        v1[0, 0, 1 + i] = value
        p1[0, 0, 1 + i] = pair1(0, value)
    for group, order in SWEEP:
        phase1(group, order)

    for i in range(4):
        for zp in range(2):
            vc[i, pl.ds(zp, 8, stride=2), :] = v1[zp, i % 2, 1 + 2 * gy + i // 2]
    for copy in field_copies:
        copy.wait_recv()
    for zp in range(2):
        for yp in range(2):
            for xp in range(2):
                for i in range(12):
                    yb, rows = window(zp, yp, i)
                    value = fw[yb, xp, rows, :] * mk[zp, i]
                    if yb == 1:
                        value = jnp.where(own_rows(zp, (8, 128)), v0[zp, yp, xp, i], value)
                    v0[zp, yp, xp, i] = value
                    if zp == 1:
                        p0[zp, yp, xp, i] = pair0(zp, value)
    for i in range(4):
        v0[0, 0, 0, 4 + i] += jnp.where(own_rows(0, (8, 128)), vc[i, 7:15, :], 0.0)

    for (group, order), (lo, hi) in zip(SWEEP, POST_ROWS):
        phase0(group, order, lo, hi)

    numer = jnp.zeros((8, 128), F32)
    denom = jnp.zeros((8, 128), F32)
    images = {}
    for zp in range(2):
        for yp in range(2):
            s = outer0(zp, yp, 4, 8)
            c = [v0[zp, yp, 0, 4:8], v0[zp, yp, 1, 4:8]]
            mine = own_rows(zp, (8, 128))
            top, bottom = 0.0, 0.0
            for xp in range(2):
                image = 26.0 * c[xp] - around0(s, c, xp)
                images[zp, yp, xp] = image
                top = top + jnp.sum(c[xp] * f0[zp, yp, xp, 4:8], axis=0)
                bottom = bottom + jnp.sum(c[xp] * image, axis=0)
            numer = numer + jnp.where(mine, top, 0.0)
            denom = denom + jnp.where(mine, bottom, 0.0)
    lower = lanes((8, 128)) < 64
    both = jnp.where(lower, numer + pltpu.roll(numer, 64, 1), denom + pltpu.roll(denom, 64, 1))
    part = jnp.sum(both, axis=0, keepdims=True)
    sb[0] = part
    first_copies = []
    for k, (c, z) in enumerate(first_group):
        copy = remote(sb.at[0], ar1.at[k], s1.at[k], r1.at[k], along_z(c, z))
        copy.start()
        first_copies.append(copy)

    for zp in range(2):
        for yp in range(2):
            for xp in range(2):
                for i in range(4):
                    rows = window(zp, yp, 4 + i)[1]
                    stage[0, xp, rows, :] = v0[zp, yp, xp, 4 + i]
                    stage[1, xp, rows, :] = images[zp, yp, xp][i]
    for t, target in enumerate((prec, imag)):
        block = jnp.concatenate([stage[t, 0, 24:88, :], stage[t, 1, 24:88, :]], axis=1)
        target[...] = permuted(block, merge).reshape(8, 8, 256)
    out_copies = [
        pltpu.make_async_copy(prec, prec_hbm, io.at[1]),
        pltpu.make_async_copy(imag, imag_hbm, io.at[2]),
    ]
    for copy in out_copies:
        copy.start()

    for copy in first_copies:
        copy.wait_recv()
    part = part + jnp.sum(ar1[...], axis=0)
    sb[1] = part
    second_copies = []
    for k, (x, y) in enumerate(second_group):
        copy = remote(sb.at[1], ar2.at[k], s2.at[k], r2.at[k], along_xy(x, y))
        copy.start()
        second_copies.append(copy)
    for copy in second_copies:
        copy.wait_recv()
    part = part + jnp.sum(ar2[...], axis=0)
    left = lanes((1, 128)) < 64
    total_n = jnp.sum(jnp.where(left, part, 0.0), axis=1, keepdims=True)
    total_d = jnp.sum(jnp.where(left, 0.0, part), axis=1, keepdims=True)
    alpha_ref[...] = total_n / total_d
    for copy in out_copies:
        copy.wait()
    for copy in rhs_copies + field_copies + coarse_copies + first_copies + second_copies:
        copy.wait_send()


def solution(mesh):
    ngz, ngy = mesh.shape["gz"], mesh.shape["gy"]
    nz = ngz // (NX_CHIPS * CORES)
    coarse = 4 * ngy - 1
    one = nz * CORES - 1
    two = NX_CHIPS * ngy - 1

    def body(right_side):
        out = jax.ShapeDtypeStruct(right_side.shape, F32)
        vm = pltpu.VMEM
        dma = pltpu.SemaphoreType.DMA
        precond, image, alpha = pl.pallas_call(
            functools.partial(kernel, ngz, ngy),
            name="cg_iteration",
            out_shape=(out, out, jax.ShapeDtypeStruct((1, 1), F32)),
            in_specs=[pl.BlockSpec(memory_space=pl.ANY)],
            out_specs=(
                pl.BlockSpec(memory_space=pl.ANY),
                pl.BlockSpec(memory_space=pl.ANY),
                pl.BlockSpec(memory_space=pltpu.VMEM),
            ),
            scratch_shapes=[
                vm((8, 8, 256), F32),
                vm((2, 64, 128), F32),
                vm((3, 2, 128, 128), F32),
                vm((2, 2, 2, 12, 8, 128), F32),
                vm((2, 2, 2, 12, 8, 128), F32),
                vm((2, 2, 2, 12, 8, 128), F32),
                vm((2, 12, 8, 128), F32),
                vm((2, 128, 128), F32),
                vm((3, 2, 128, 128), F32),
                vm((32, 128), F32),
                vm((ngy, 64, 128), F32),
                vm((2, 2, 2 * ngy, 8, 128), F32),
                vm((2, 2, 2 * ngy + 2, 8, 128), F32),
                vm((2, 2, 2 * ngy + 2, 8, 128), F32),
                vm((2, ngy, 8, 128), F32),
                vm((2, ngy + 2, 8, 128), F32),
                vm((4, 16, 128), F32),
                vm((2, 2, 128, 128), F32),
                vm((8, 8, 256), F32),
                vm((8, 8, 256), F32),
                vm((2, 1, 128), F32),
                vm((one, 1, 128), F32),
                vm((two, 1, 128), F32),
                dma((3,)), dma((8,)), dma((8,)), dma((8,)), dma((8,)), dma((coarse,)), dma((coarse,)),
                dma((one,)), dma((one,)), dma((two,)), dma((two,)),
            ],
            compiler_params=pltpu.CompilerParams(collective_id=0, has_side_effects=True),
        )(right_side)
        return alpha[:, :, None] * precond, right_side - alpha[:, :, None] * image

    return jax.shard_map(
        body,
        mesh=mesh,
        in_specs=(P("gz", "gy", None),),
        out_specs=(P("gz", "gy", None), P("gz", "gy", None)),
        check_vma=False,
    )
```

```python
import functools

import jax
import jax.numpy as jnp
from jax import lax
from jax.experimental import pallas as pl
from jax.experimental.pallas import tpu as pltpu
from jax.sharding import PartitionSpec as P

MESH = pl.DeviceIdType.MESH
F32 = jnp.float32
INV = 1.0 / 26.0
NX_CHIPS = 4
CORES = 2

SWEEP = [
    ((0, 0), (0, 1)),
    ((0, 1), (0, 1)),
    ((1, 0), (0, 1)),
    ((1, 1), (0, 1, 0)),
    ((1, 0), (1, 0)),
    ((0, 1), (1, 0)),
    ((0, 0), (1, 0)),
]
PRE_ROWS = [(1, 11), (1, 10), (2, 10), (2, 9), (3, 9), (3, 8), (4, 8)]
POST_ROWS = [(1, 12), (1, 11), (2, 11), (2, 10), (3, 10), (3, 9), (4, 9)]


def lanes(shape):
    return lax.broadcasted_iota(jnp.int32, shape, len(shape) - 1)


def sublanes(shape):
    return lax.broadcasted_iota(jnp.int32, shape, len(shape) - 2)


def from_left(u, step=1):
    return jnp.where(lanes(u.shape) >= step, pltpu.roll(u, step, u.ndim - 1), 0.0)


def from_right(u, step=1):
    return jnp.where(lanes(u.shape) < 128 - step, pltpu.roll(u, 128 - step, u.ndim - 1), 0.0)


def both_sides(u, step=1):
    return from_left(u, step) + from_right(u, step)


def down(u):
    return pltpu.roll(u, 1, u.ndim - 2)


def up(u):
    return pltpu.roll(u, 7, u.ndim - 2)


def remote(src, dst, send, recv, where):
    copy = pltpu.make_async_remote_copy(
        src_ref=src, dst_ref=dst, send_sem=send, recv_sem=recv, device_id=where, device_id_type=MESH
    )
    return copy


def kernel(
    ngz, ngy, r_hbm, prec_hbm, imag_hbm, alpha_ref,
    rin, ownr, rd, f0, v0, p0, mk, own, fw, dcb, dall, f1, v1, p1, f2, v2, vc, stage, prec, imag, sb, ar1, ar2,
    near, far, beside, io, rs, rr, fs, fr, cs, cr, s1, r1, s2, r2,
):
    gz = lax.axis_index("gz")
    gy = lax.axis_index("gy")
    nz = ngz // (NX_CHIPS * CORES)
    core = lax.rem(gz, CORES)
    chip_x = lax.rem(gz // CORES, NX_CHIPS)
    chip_z = gz // (CORES * NX_CHIPS)

    def at(dz, dy):
        return (lax.rem(gz + dz % ngz, ngz), lax.rem(gy + dy % ngy, ngy))

    def along_z(dc, dz):
        z = lax.rem(chip_z + dz % nz, nz)
        return ((z * NX_CHIPS + chip_x) * CORES + lax.rem(core + dc % CORES, CORES), gy)

    def along_xy(dx, dy):
        x = lax.rem(chip_x + dx % NX_CHIPS, NX_CHIPS)
        return ((chip_z * NX_CHIPS + x) * CORES + core, lax.rem(gy + dy % ngy, ngy))

    coarse_sends = [
        (slot, dz, dy)
        for dy in sorted(range(ngy), key=lambda d: -min(d, ngy - d))
        for slot, dz in ((2, 0), (1, 1), (3, -1), (0, 2))
        if not (dz == 0 and dy == 0)
    ]
    first_group = [(c, z) for z in range(nz) for c in range(CORES) if (c, z) != (0, 0)]
    first_group.sort(key=lambda g: -min(g[1], nz - g[1]))
    second_group = [(x, y) for y in range(ngy) for x in range(NX_CHIPS) if (x, y) != (0, 0)]
    second_group.sort(key=lambda g: -min(g[1], ngy - g[1]) - min(g[0], NX_CHIPS - g[0]))
    halo = [(dz, dy) for dz in (0, 1, -1) for dy in (0, 1, -1) if (dz, dy) != (0, 0)]

    load = pltpu.make_async_copy(r_hbm, rin, io.at[0])
    load.start()

    barrier = pltpu.get_barrier_semaphore()
    for dz, dy in halo:
        pl.semaphore_signal(barrier, inc=1, device_id=at(-dz, -dy), device_id_type=MESH)

    def tell(semaphore, offsets):
        for dz, dy in offsets:
            pl.semaphore_signal(semaphore, inc=1, device_id=at(dz, dy), device_id_type=MESH)

    reach = 4
    rounds = []
    while reach < ngz // 2 + 1:
        rounds.append([(reach, 0), (-reach, 0)])
        reach *= 2
    done = []

    def advance():
        k = len(done)
        if 0 < k <= len(rounds):
            pl.semaphore_wait(far.at[k - 1], 2)
        if k < len(rounds):
            tell(far.at[k], rounds[k])
        done.append(k)

    row = lax.broadcasted_iota(jnp.int32, (256, 256), 0)
    col = lax.broadcasted_iota(jnp.int32, (256, 256), 1)
    split = (row == jnp.where(col < 128, 2 * col, 2 * col - 255)).astype(F32).astype(jnp.bfloat16)
    merge = (col == jnp.where(row < 128, 2 * row, 2 * row - 255)).astype(F32).astype(jnp.bfloat16)

    def permuted(block, matrix):
        high = block.astype(jnp.bfloat16)
        rest = block - high.astype(F32)
        middle = rest.astype(jnp.bfloat16)
        low = (rest - middle.astype(F32)).astype(jnp.bfloat16)
        moved = [
            lax.dot_general(part, matrix, (((1,), (0,)), ((), ())), preferred_element_type=F32)
            for part in (high, middle, low)
        ]
        return (moved[0] + moved[1]) + moved[2]

    for yb in range(3):
        rd[yb, :, 0:8, :] = jnp.zeros((2, 8, 128), F32)
        rd[yb, :, 112:128, :] = jnp.zeros((2, 16, 128), F32)
        fw[yb, :, 120:128, :] = jnp.zeros((2, 8, 128), F32)
    fw[1, :, 24:88, :] = jnp.zeros((2, 64, 128), F32)
    dall[:, 0:8, :] = jnp.zeros((ngy, 8, 128), F32)
    v0[...] = jnp.zeros(v0.shape, F32)
    p0[...] = jnp.zeros(p0.shape, F32)
    v1[...] = jnp.zeros(v1.shape, F32)
    p1[...] = jnp.zeros(p1.shape, F32)
    v2[...] = jnp.zeros(v2.shape, F32)

    load.wait()
    both = permuted(rin[...].reshape(64, 256), split)
    for xp in range(2):
        part = both[:, 128 * xp : 128 * xp + 128]
        ownr[xp] = part
        rd[1, xp, 24:88, :] = part

    sub = sublanes((8, 128))
    for zp in range(2):
        z = gz * 8 + 2 * sub - (2 + zp)
        z_in = ((z >= 0) & (z < ngz * 8)).astype(F32)
        low = jnp.where(gy > 0, 1.0, 0.0).astype(F32)
        high = jnp.where(gy < ngy - 1, 1.0, 0.0).astype(F32)
        mk[zp, 0:4] = jnp.broadcast_to(z_in * low, (4, 8, 128))
        mk[zp, 4:8] = jnp.broadcast_to(z_in, (4, 8, 128))
        mk[zp, 8:12] = jnp.broadcast_to(z_in * high, (4, 8, 128))

    def own_rows(zp, shape):
        s = sublanes(shape)
        return (s >= 1 + zp) & (s < 5 + zp)

    pl.semaphore_wait(barrier, len(halo))

    def border(source, target, rows, sends, arrivals):
        copies = []
        for k, (dz, dy) in enumerate(halo):
            z_from, count, z_to = rows[dz]
            copy = remote(
                source.at[:, pl.ds(8 * z_from, 8 * count), :],
                target.at[1 - dy, :, pl.ds(8 * z_to, 8 * count), :],
                sends.at[k], arrivals.at[k], at(dz, dy),
            )
            copy.start()
            copies.append(copy)
        return copies

    rhs_copies = border(ownr, rd, {0: (0, 8, 3), 1: (6, 2, 1), -1: (0, 3, 11)}, rs, rr)
    for copy in rhs_copies:
        copy.wait_recv()
    tell(near, [(0, 2), (0, -2), (2, 0), (-2, 0)])

    def window(zp, yp, i):
        return i // 4, pl.ds(8 * (1 - zp) + 2 * (i % 4) + yp, 8, stride=16)

    for zp in range(2):
        for yp in range(2):
            for xp in range(2):
                for i in range(12):
                    yb, rows = window(zp, yp, i)
                    f0[zp, yp, xp, i] = rd[yb, xp, rows, :]

    def pair0(zp, c):
        return c + (down(c) if zp == 0 else up(c))

    def outer0(zp, yp, lo, hi):
        a = -1 if yp == 0 else 0
        sums = []
        for xp in range(2):
            s = v0[zp, 1 - yp, xp, lo + a : hi + a] + v0[zp, 1 - yp, xp, lo + a + 1 : hi + a + 1]
            q = p0[1 - zp, 1 - yp, xp, lo + a : hi + a] + p0[1 - zp, 1 - yp, xp, lo + a + 1 : hi + a + 1]
            sums.append(s + q + p0[1 - zp, yp, xp, lo:hi])
        return sums

    def around0(s, c, xp):
        other = s[1 - xp] + c[1 - xp]
        return s[xp] + (other + (from_left(other) if xp == 0 else from_right(other)))

    def phase0(group, order, lo, hi):
        zp, yp = group
        s = outer0(zp, yp, lo, hi)
        c = [v0[zp, yp, 0, lo:hi], v0[zp, yp, 1, lo:hi]]
        scale = mk[zp, lo:hi] * INV
        for xp in order:
            c[xp] = (around0(s, c, xp) + f0[zp, yp, xp, lo:hi]) * scale
        for xp in range(2):
            v0[zp, yp, xp, lo:hi] = c[xp]
            p0[zp, yp, xp, lo:hi] = pair0(zp, c[xp])

    for (group, order), (lo, hi) in zip(SWEEP, PRE_ROWS):
        phase0(group, order, lo, hi)

    s = outer0(0, 0, 4, 8)
    c = [v0[0, 0, 0, 4:8], v0[0, 0, 1, 4:8]]
    defect = up(f0[0, 0, 0, 4:8] - (26.0 * c[0] - around0(s, c, 0)))
    for i in range(4):
        dcb[pl.ds(i, 8, stride=4), :] = defect[i]
    for zp in range(2):
        for yp in range(2):
            for xp in range(2):
                for i in range(4, 8):
                    own[xp, window(zp, yp, i)[1], :] = v0[zp, yp, xp, i]
    pl.semaphore_wait(near, 4)
    coarse_copies = []
    for k, (slot, dz, dy) in enumerate(coarse_sends):
        first, count = (8, 8) if slot == 0 else (0, 16)
        copy = remote(
            dcb.at[pl.ds(first, count), :], dall.at[gy, pl.ds(16 * slot + first, count), :],
            cs.at[k], cr.at[k], at(dz, dy),
        )
        copy.start()
        coarse_copies.append(copy)
    field_copies = border(own, fw, {0: (3, 8, 3), 1: (8, 3, 0), -1: (3, 4, 11)}, fs, fr)
    dall[gy, 32:48, :] = dcb[0:16, :]

    for _ in range(3):
        advance()
    for copy in coarse_copies:
        copy.wait_recv()
    tell(beside, [(-1, 0)])

    n1 = 2 * ngy
    for zp in range(2):
        for yp in range(2):
            for i in range(n1):
                f1[zp, yp, i] = dall[i // 2, pl.ds(2 * (i % 2) + yp + 4 * zp, 8, stride=8), :]

    scale1 = []
    for zp in range(2):
        z = gz * 4 + 2 * sub - (8 - zp)
        scale1.append(jnp.where((z >= 0) & (z < ngz * 4), INV, 0.0).astype(F32)[None])

    def pair1(zp, c):
        return c + (up(c) if zp == 0 else down(c))

    def outer1(zp, yp):
        a = 0 if yp == 0 else 1
        s = v1[zp, 1 - yp, a : a + n1] + v1[zp, 1 - yp, a + 1 : a + 1 + n1]
        q = p1[1 - zp, 1 - yp, a : a + n1] + p1[1 - zp, 1 - yp, a + 1 : a + 1 + n1]
        return s + q + p1[1 - zp, yp, 1 : 1 + n1]

    def phase1(group, order):
        zp, yp = group
        s = outer1(zp, yp)
        c = v1[zp, yp, 1 : 1 + n1]
        base = s + f1[zp, yp]
        parity = lax.rem(lanes(c.shape), 2)
        for xp in order:
            c = jnp.where(parity == xp, (base + both_sides(s + c)) * scale1[zp], c)
        v1[zp, yp, 1 : 1 + n1] = c
        p1[zp, yp, 1 : 1 + n1] = pair1(zp, c)

    for group, order in SWEEP:
        phase1(group, order)
    advance()

    n2 = ngy
    s = outer1(0, 0)
    c = v1[0, 0, 1 : 1 + n1]
    even = lax.rem(lanes(c.shape), 2) == 0
    defect = jnp.where(even, f1[0, 0] - (26.0 * c - (s + both_sides(s + c))), 0.0)
    for i in range(n1):
        f2[i % 2, i // 2] = defect[i]
    z = gz * 2 + sub - 4
    scale2 = jnp.where((z >= 0) & (z < ngz * 2), INV, 0.0).astype(F32)[None]

    for group, order in SWEEP:
        zp, yp = group
        a = 0 if yp == 0 else 1
        c = v2[yp, 1 : 1 + n2]
        side = v2[1 - yp, a : a + n2] + v2[1 - yp, a + 1 : a + 1 + n2]
        column = side + c
        s = side + (down(column) + up(column))
        base = s + f2[yp]
        layer = lax.rem(sublanes(c.shape), 2) == zp
        place = lax.rem(lanes(c.shape), 4)
        for xp in order:
            c = jnp.where(layer & (place == 2 * xp), (base + both_sides(s + c, 2)) * scale2, c)
        v2[yp, 1 : 1 + n2] = c

    held = sublanes((8, 128))
    mine = (held >= 4) & (held < 6)
    for i in range(n1):
        value = v1[0, 0, 1 + i] + jnp.where(mine, v2[i % 2, 1 + i // 2], 0.0)
        v1[0, 0, 1 + i] = value
        p1[0, 0, 1 + i] = pair1(0, value)
    for group, order in SWEEP:
        phase1(group, order)

    while len(done) <= len(rounds):
        advance()
    pl.semaphore_wait(beside, 1)

    for i in range(4):
        for zp in range(2):
            vc[i, pl.ds(zp, 8, stride=2), :] = v1[zp, i % 2, 1 + 2 * gy + i // 2]
    for copy in field_copies:
        copy.wait_recv()
    for zp in range(2):
        for yp in range(2):
            for xp in range(2):
                for i in range(12):
                    yb, rows = window(zp, yp, i)
                    value = fw[yb, xp, rows, :] * mk[zp, i]
                    if yb == 1:
                        value = jnp.where(own_rows(zp, (8, 128)), v0[zp, yp, xp, i], value)
                    v0[zp, yp, xp, i] = value
                    if zp == 1:
                        p0[zp, yp, xp, i] = pair0(zp, value)
    for i in range(4):
        v0[0, 0, 0, 4 + i] += jnp.where(own_rows(0, (8, 128)), vc[i, 7:15, :], 0.0)

    for (group, order), (lo, hi) in zip(SWEEP, POST_ROWS):
        phase0(group, order, lo, hi)

    numer = jnp.zeros((8, 128), F32)
    denom = jnp.zeros((8, 128), F32)
    images = {}
    for zp in range(2):
        for yp in range(2):
            s = outer0(zp, yp, 4, 8)
            c = [v0[zp, yp, 0, 4:8], v0[zp, yp, 1, 4:8]]
            mine = own_rows(zp, (8, 128))
            top, bottom = 0.0, 0.0
            for xp in range(2):
                image = 26.0 * c[xp] - around0(s, c, xp)
                images[zp, yp, xp] = image
                top = top + jnp.sum(c[xp] * f0[zp, yp, xp, 4:8], axis=0)
                bottom = bottom + jnp.sum(c[xp] * image, axis=0)
            numer = numer + jnp.where(mine, top, 0.0)
            denom = denom + jnp.where(mine, bottom, 0.0)
    lower = lanes((8, 128)) < 64
    both = jnp.where(lower, numer + pltpu.roll(numer, 64, 1), denom + pltpu.roll(denom, 64, 1))
    part = jnp.sum(both, axis=0, keepdims=True)
    sb[0] = part
    first_copies = []
    for k, (c, z) in enumerate(first_group):
        copy = remote(sb.at[0], ar1.at[k], s1.at[k], r1.at[k], along_z(c, z))
        copy.start()
        first_copies.append(copy)

    for zp in range(2):
        for yp in range(2):
            for xp in range(2):
                for i in range(4):
                    rows = window(zp, yp, 4 + i)[1]
                    stage[0, xp, rows, :] = v0[zp, yp, xp, 4 + i]
                    stage[1, xp, rows, :] = images[zp, yp, xp][i]
    for t, target in enumerate((prec, imag)):
        block = jnp.concatenate([stage[t, 0, 24:88, :], stage[t, 1, 24:88, :]], axis=1)
        target[...] = permuted(block, merge).reshape(8, 8, 256)
    out_copies = [
        pltpu.make_async_copy(prec, prec_hbm, io.at[1]),
        pltpu.make_async_copy(imag, imag_hbm, io.at[2]),
    ]
    for copy in out_copies:
        copy.start()

    for copy in first_copies:
        copy.wait_recv()
    part = part + jnp.sum(ar1[...], axis=0)
    sb[1] = part
    second_copies = []
    for k, (x, y) in enumerate(second_group):
        copy = remote(sb.at[1], ar2.at[k], s2.at[k], r2.at[k], along_xy(x, y))
        copy.start()
        second_copies.append(copy)
    for copy in second_copies:
        copy.wait_recv()
    part = part + jnp.sum(ar2[...], axis=0)
    left = lanes((1, 128)) < 64
    total_n = jnp.sum(jnp.where(left, part, 0.0), axis=1, keepdims=True)
    total_d = jnp.sum(jnp.where(left, 0.0, part), axis=1, keepdims=True)
    alpha_ref[...] = total_n / total_d
    for copy in out_copies:
        copy.wait()
    for copy in rhs_copies + field_copies + coarse_copies + first_copies + second_copies:
        copy.wait_send()


def solution(mesh):
    ngz, ngy = mesh.shape["gz"], mesh.shape["gy"]
    nz = ngz // (NX_CHIPS * CORES)
    coarse = 4 * ngy - 1
    one = nz * CORES - 1
    two = NX_CHIPS * ngy - 1

    def body(right_side):
        out = jax.ShapeDtypeStruct(right_side.shape, F32)
        vm = pltpu.VMEM
        dma = pltpu.SemaphoreType.DMA
        precond, image, alpha = pl.pallas_call(
            functools.partial(kernel, ngz, ngy),
            name="cg_iteration",
            out_shape=(pltpu.VMEM(right_side.shape, F32), pltpu.VMEM(right_side.shape, F32), jax.ShapeDtypeStruct((1, 1), F32)),
            in_specs=[pl.BlockSpec(memory_space=pltpu.HBM)],
            out_specs=(
                pl.BlockSpec(memory_space=pl.ANY),
                pl.BlockSpec(memory_space=pl.ANY),
                pl.BlockSpec(memory_space=pltpu.VMEM),
            ),
            scratch_shapes=[
                vm((8, 8, 256), F32),
                vm((2, 64, 128), F32),
                vm((3, 2, 128, 128), F32),
                vm((2, 2, 2, 12, 8, 128), F32),
                vm((2, 2, 2, 12, 8, 128), F32),
                vm((2, 2, 2, 12, 8, 128), F32),
                vm((2, 12, 8, 128), F32),
                vm((2, 128, 128), F32),
                vm((3, 2, 128, 128), F32),
                vm((32, 128), F32),
                vm((ngy, 64, 128), F32),
                vm((2, 2, 2 * ngy, 8, 128), F32),
                vm((2, 2, 2 * ngy + 2, 8, 128), F32),
                vm((2, 2, 2 * ngy + 2, 8, 128), F32),
                vm((2, ngy, 8, 128), F32),
                vm((2, ngy + 2, 8, 128), F32),
                vm((4, 16, 128), F32),
                vm((2, 2, 128, 128), F32),
                vm((8, 8, 256), F32),
                vm((8, 8, 256), F32),
                vm((2, 1, 128), F32),
                vm((one, 1, 128), F32),
                vm((two, 1, 128), F32),
                pltpu.SemaphoreType.REGULAR, pltpu.SemaphoreType.REGULAR((8,)), pltpu.SemaphoreType.REGULAR,
                dma((3,)), dma((8,)), dma((8,)), dma((8,)), dma((8,)), dma((coarse,)), dma((coarse,)),
                dma((one,)), dma((one,)), dma((two,)), dma((two,)),
            ],
            compiler_params=pltpu.CompilerParams(collective_id=0, has_side_effects=True, vmem_limit_bytes=60000000),
        )(right_side)
        return alpha[:, :, None] * precond, right_side - alpha[:, :, None] * image

    return jax.shard_map(
        body,
        mesh=mesh,
        in_specs=(P("gz", "gy", None),),
        out_specs=(P("gz", "gy", None), P("gz", "gy", None)),
        check_vma=False,
    )
```

```python
import functools

import jax
import jax.numpy as jnp
from jax import lax
from jax.experimental import pallas as pl
from jax.experimental.pallas import tpu as pltpu
from jax.sharding import PartitionSpec as P

MESH = pl.DeviceIdType.MESH
F32 = jnp.float32
INV = 1.0 / 26.0
NX_CHIPS = 4
CORES = 2

SWEEP = [
    ((0, 0), (0, 1)),
    ((0, 1), (0, 1)),
    ((1, 0), (0, 1)),
    ((1, 1), (0, 1, 0)),
    ((1, 0), (1, 0)),
    ((0, 1), (1, 0)),
    ((0, 0), (1, 0)),
]
PRE_ROWS = [(1, 11), (1, 10), (2, 10), (2, 9), (3, 9), (3, 8), (4, 8)]
POST_ROWS = [(1, 12), (1, 11), (2, 11), (2, 10), (3, 10), (3, 9), (4, 9)]


def lanes(shape):
    return lax.broadcasted_iota(jnp.int32, shape, len(shape) - 1)


def sublanes(shape):
    return lax.broadcasted_iota(jnp.int32, shape, len(shape) - 2)


def from_left(u, step=1):
    return jnp.where(lanes(u.shape) >= step, pltpu.roll(u, step, u.ndim - 1), 0.0)


def from_right(u, step=1):
    return jnp.where(lanes(u.shape) < 128 - step, pltpu.roll(u, 128 - step, u.ndim - 1), 0.0)


def both_sides(u, step=1):
    return from_left(u, step) + from_right(u, step)


def down(u):
    return pltpu.roll(u, 1, u.ndim - 2)


def up(u):
    return pltpu.roll(u, 7, u.ndim - 2)


def remote(src, dst, send, recv, where):
    copy = pltpu.make_async_remote_copy(
        src_ref=src, dst_ref=dst, send_sem=send, recv_sem=recv, device_id=where, device_id_type=MESH
    )
    return copy


def kernel(
    ngz, ngy, r_hbm, prec_hbm, imag_hbm, alpha_ref,
    rin, ownr, rd, f0, v0, p0, mk, own, fw, dcb, dall, f1, v1, p1, f2, v2, vc, stage, prec, imag, sb, ar1, ar2,
    near, far, beside, io, rs, rr, fs, fr, cs, cr, s1, r1, s2, r2,
):
    gz = lax.axis_index("gz")
    gy = lax.axis_index("gy")
    nz = ngz // (NX_CHIPS * CORES)
    core = lax.rem(gz, CORES)
    chip_x = lax.rem(gz // CORES, NX_CHIPS)
    chip_z = gz // (CORES * NX_CHIPS)

    def at(dz, dy):
        return (lax.rem(gz + dz % ngz, ngz), lax.rem(gy + dy % ngy, ngy))

    def along_z(dc, dz):
        z = lax.rem(chip_z + dz % nz, nz)
        return ((z * NX_CHIPS + chip_x) * CORES + lax.rem(core + dc % CORES, CORES), gy)

    def along_xy(dx, dy):
        x = lax.rem(chip_x + dx % NX_CHIPS, NX_CHIPS)
        return ((chip_z * NX_CHIPS + x) * CORES + core, lax.rem(gy + dy % ngy, ngy))

    coarse_sends = [
        (slot, dz, dy)
        for dy in sorted(range(ngy), key=lambda d: (min(d, ngy - d) > 2, -min(d, ngy - d)))
        for slot, dz in ((2, 0), (1, 1), (3, -1), (0, 2))
        if not (dz == 0 and dy == 0)
    ]
    first_group = [(c, z) for z in range(nz) for c in range(CORES) if (c, z) != (0, 0)]
    first_group.sort(key=lambda g: -min(g[1], nz - g[1]))
    second_group = [(x, y) for y in range(ngy) for x in range(NX_CHIPS) if (x, y) != (0, 0)]
    second_group.sort(key=lambda g: -min(g[1], ngy - g[1]) - min(g[0], NX_CHIPS - g[0]))
    halo = [(dz, dy) for dz in (0, 1, -1) for dy in (0, 1, -1) if (dz, dy) != (0, 0)]

    load = pltpu.make_async_copy(r_hbm, rin, io.at[0])
    load.start()

    barrier = pltpu.get_barrier_semaphore()
    greeted = [at(dz, dy) for dz, dy in halo]
    greeted += [along_z(0, z) for z in (1, -1, 2, -2) if z % nz]
    greeted += [along_xy(x, 0) for x in range(1, NX_CHIPS)]

    def tell(semaphore, devices):
        for device in devices:
            pl.semaphore_signal(semaphore, inc=1, device_id=device, device_id_type=MESH)

    tell(barrier, greeted)
    two_away = [along_z(0, z) for z in (2, -2) if z % nz]
    three_away = [along_z(0, z) for z in (3, -3) if z % nz]

    row = lax.broadcasted_iota(jnp.int32, (256, 256), 0)
    col = lax.broadcasted_iota(jnp.int32, (256, 256), 1)
    split = (row == jnp.where(col < 128, 2 * col, 2 * col - 255)).astype(F32).astype(jnp.bfloat16)
    merge = (col == jnp.where(row < 128, 2 * row, 2 * row - 255)).astype(F32).astype(jnp.bfloat16)

    def permuted(block, matrix):
        high = block.astype(jnp.bfloat16)
        rest = block - high.astype(F32)
        middle = rest.astype(jnp.bfloat16)
        low = (rest - middle.astype(F32)).astype(jnp.bfloat16)
        moved = [
            lax.dot_general(part, matrix, (((1,), (0,)), ((), ())), preferred_element_type=F32)
            for part in (high, middle, low)
        ]
        return (moved[0] + moved[1]) + moved[2]

    for yb in range(3):
        rd[yb, :, 0:8, :] = jnp.zeros((2, 8, 128), F32)
        rd[yb, :, 112:128, :] = jnp.zeros((2, 16, 128), F32)
        fw[yb, :, 120:128, :] = jnp.zeros((2, 8, 128), F32)
    fw[1, :, 24:88, :] = jnp.zeros((2, 64, 128), F32)
    dall[:, 0:8, :] = jnp.zeros((ngy, 8, 128), F32)
    v0[...] = jnp.zeros(v0.shape, F32)
    p0[...] = jnp.zeros(p0.shape, F32)
    v1[...] = jnp.zeros(v1.shape, F32)
    p1[...] = jnp.zeros(p1.shape, F32)
    v2[...] = jnp.zeros(v2.shape, F32)

    load.wait()
    both = permuted(rin[...].reshape(64, 256), split)
    for xp in range(2):
        part = both[:, 128 * xp : 128 * xp + 128]
        ownr[xp] = part
        rd[1, xp, 24:88, :] = part

    sub = sublanes((8, 128))
    for zp in range(2):
        z = gz * 8 + 2 * sub - (2 + zp)
        z_in = ((z >= 0) & (z < ngz * 8)).astype(F32)
        low = jnp.where(gy > 0, 1.0, 0.0).astype(F32)
        high = jnp.where(gy < ngy - 1, 1.0, 0.0).astype(F32)
        mk[zp, 0:4] = jnp.broadcast_to(z_in * low, (4, 8, 128))
        mk[zp, 4:8] = jnp.broadcast_to(z_in, (4, 8, 128))
        mk[zp, 8:12] = jnp.broadcast_to(z_in * high, (4, 8, 128))

    def own_rows(zp, shape):
        s = sublanes(shape)
        return (s >= 1 + zp) & (s < 5 + zp)

    pl.semaphore_wait(barrier, len(greeted))

    def border(source, target, rows, sends, arrivals):
        copies = []
        for k, (dz, dy) in enumerate(halo):
            z_from, count, z_to = rows[dz]
            copy = remote(
                source.at[:, pl.ds(8 * z_from, 8 * count), :],
                target.at[1 - dy, :, pl.ds(8 * z_to, 8 * count), :],
                sends.at[k], arrivals.at[k], at(dz, dy),
            )
            copy.start()
            copies.append(copy)
        return copies

    tell(far.at[0], two_away)
    rhs_copies = border(ownr, rd, {0: (0, 8, 3), 1: (6, 2, 1), -1: (0, 3, 11)}, rs, rr)
    for copy in rhs_copies:
        copy.wait_recv()
    tell(near, [at(0, 2), at(0, -2)])
    if two_away:
        pl.semaphore_wait(far.at[0], len(two_away))
    tell(far.at[1], three_away)

    def window(zp, yp, i):
        return i // 4, pl.ds(8 * (1 - zp) + 2 * (i % 4) + yp, 8, stride=16)

    for zp in range(2):
        for yp in range(2):
            for xp in range(2):
                for i in range(12):
                    yb, rows = window(zp, yp, i)
                    f0[zp, yp, xp, i] = rd[yb, xp, rows, :]

    def pair0(zp, c):
        return c + (down(c) if zp == 0 else up(c))

    def outer0(zp, yp, lo, hi):
        a = -1 if yp == 0 else 0
        sums = []
        for xp in range(2):
            s = v0[zp, 1 - yp, xp, lo + a : hi + a] + v0[zp, 1 - yp, xp, lo + a + 1 : hi + a + 1]
            q = p0[1 - zp, 1 - yp, xp, lo + a : hi + a] + p0[1 - zp, 1 - yp, xp, lo + a + 1 : hi + a + 1]
            sums.append(s + q + p0[1 - zp, yp, xp, lo:hi])
        return sums

    def around0(s, c, xp):
        other = s[1 - xp] + c[1 - xp]
        return s[xp] + (other + (from_left(other) if xp == 0 else from_right(other)))

    def phase0(group, order, lo, hi):
        zp, yp = group
        s = outer0(zp, yp, lo, hi)
        c = [v0[zp, yp, 0, lo:hi], v0[zp, yp, 1, lo:hi]]
        scale = mk[zp, lo:hi] * INV
        for xp in order:
            c[xp] = (around0(s, c, xp) + f0[zp, yp, xp, lo:hi]) * scale
        for xp in range(2):
            v0[zp, yp, xp, lo:hi] = c[xp]
            p0[zp, yp, xp, lo:hi] = pair0(zp, c[xp])

    for (group, order), (lo, hi) in zip(SWEEP, PRE_ROWS):
        phase0(group, order, lo, hi)

    s = outer0(0, 0, 4, 8)
    c = [v0[0, 0, 0, 4:8], v0[0, 0, 1, 4:8]]
    defect = up(f0[0, 0, 0, 4:8] - (26.0 * c[0] - around0(s, c, 0)))
    for i in range(4):
        dcb[pl.ds(i, 8, stride=4), :] = defect[i]
    for zp in range(2):
        for yp in range(2):
            for xp in range(2):
                for i in range(4, 8):
                    own[xp, window(zp, yp, i)[1], :] = v0[zp, yp, xp, i]
    coarse_copies = []
    reached = sum(min(dy, ngy - dy) <= 2 for _, _, dy in coarse_sends) % len(coarse_sends)
    for k, (slot, dz, dy) in enumerate(coarse_sends):
        if k == reached:
            pl.semaphore_wait(near, 2)
        first, count = (8, 8) if slot == 0 else (0, 16)
        copy = remote(
            dcb.at[pl.ds(first, count), :], dall.at[gy, pl.ds(16 * slot + first, count), :],
            cs.at[k], cr.at[k], at(dz, dy),
        )
        copy.start()
        coarse_copies.append(copy)
    field_copies = border(own, fw, {0: (3, 8, 3), 1: (8, 3, 0), -1: (3, 4, 11)}, fs, fr)
    dall[gy, 32:48, :] = dcb[0:16, :]

    for copy in coarse_copies:
        copy.wait_recv()
    if three_away:
        pl.semaphore_wait(far.at[1], len(three_away))
    tell(beside, [along_z(1, 0)])

    n1 = 2 * ngy
    for zp in range(2):
        for yp in range(2):
            for i in range(n1):
                f1[zp, yp, i] = dall[i // 2, pl.ds(2 * (i % 2) + yp + 4 * zp, 8, stride=8), :]

    scale1 = []
    for zp in range(2):
        z = gz * 4 + 2 * sub - (8 - zp)
        scale1.append(jnp.where((z >= 0) & (z < ngz * 4), INV, 0.0).astype(F32)[None])

    def pair1(zp, c):
        return c + (up(c) if zp == 0 else down(c))

    def outer1(zp, yp):
        a = 0 if yp == 0 else 1
        s = v1[zp, 1 - yp, a : a + n1] + v1[zp, 1 - yp, a + 1 : a + 1 + n1]
        q = p1[1 - zp, 1 - yp, a : a + n1] + p1[1 - zp, 1 - yp, a + 1 : a + 1 + n1]
        return s + q + p1[1 - zp, yp, 1 : 1 + n1]

    def phase1(group, order):
        zp, yp = group
        s = outer1(zp, yp)
        c = v1[zp, yp, 1 : 1 + n1]
        base = s + f1[zp, yp]
        parity = lax.rem(lanes(c.shape), 2)
        for xp in order:
            c = jnp.where(parity == xp, (base + both_sides(s + c)) * scale1[zp], c)
        v1[zp, yp, 1 : 1 + n1] = c
        p1[zp, yp, 1 : 1 + n1] = pair1(zp, c)

    for group, order in SWEEP:
        phase1(group, order)

    n2 = ngy
    s = outer1(0, 0)
    c = v1[0, 0, 1 : 1 + n1]
    even = lax.rem(lanes(c.shape), 2) == 0
    defect = jnp.where(even, f1[0, 0] - (26.0 * c - (s + both_sides(s + c))), 0.0)
    for i in range(n1):
        f2[i % 2, i // 2] = defect[i]
    z = gz * 2 + sub - 4
    scale2 = jnp.where((z >= 0) & (z < ngz * 2), INV, 0.0).astype(F32)[None]

    for group, order in SWEEP:
        zp, yp = group
        a = 0 if yp == 0 else 1
        c = v2[yp, 1 : 1 + n2]
        side = v2[1 - yp, a : a + n2] + v2[1 - yp, a + 1 : a + 1 + n2]
        column = side + c
        s = side + (down(column) + up(column))
        base = s + f2[yp]
        layer = lax.rem(sublanes(c.shape), 2) == zp
        place = lax.rem(lanes(c.shape), 4)
        for xp in order:
            c = jnp.where(layer & (place == 2 * xp), (base + both_sides(s + c, 2)) * scale2, c)
        v2[yp, 1 : 1 + n2] = c

    held = sublanes((8, 128))
    mine = (held >= 4) & (held < 6)
    for i in range(n1):
        value = v1[0, 0, 1 + i] + jnp.where(mine, v2[i % 2, 1 + i // 2], 0.0)
        v1[0, 0, 1 + i] = value
        p1[0, 0, 1 + i] = pair1(0, value)
    for group, order in SWEEP:
        phase1(group, order)

    pl.semaphore_wait(beside, 1)

    for i in range(4):
        for zp in range(2):
            vc[i, pl.ds(zp, 8, stride=2), :] = v1[zp, i % 2, 1 + 2 * gy + i // 2]
    for copy in field_copies:
        copy.wait_recv()
    for zp in range(2):
        for yp in range(2):
            for xp in range(2):
                for i in range(12):
                    yb, rows = window(zp, yp, i)
                    value = fw[yb, xp, rows, :] * mk[zp, i]
                    if yb == 1:
                        value = jnp.where(own_rows(zp, (8, 128)), v0[zp, yp, xp, i], value)
                    v0[zp, yp, xp, i] = value
                    if zp == 1:
                        p0[zp, yp, xp, i] = pair0(zp, value)
    for i in range(4):
        v0[0, 0, 0, 4 + i] += jnp.where(own_rows(0, (8, 128)), vc[i, 7:15, :], 0.0)

    for (group, order), (lo, hi) in zip(SWEEP, POST_ROWS):
        phase0(group, order, lo, hi)

    numer = jnp.zeros((8, 128), F32)
    denom = jnp.zeros((8, 128), F32)
    images = {}
    for zp in range(2):
        for yp in range(2):
            s = outer0(zp, yp, 4, 8)
            c = [v0[zp, yp, 0, 4:8], v0[zp, yp, 1, 4:8]]
            mine = own_rows(zp, (8, 128))
            top, bottom = 0.0, 0.0
            for xp in range(2):
                image = 26.0 * c[xp] - around0(s, c, xp)
                images[zp, yp, xp] = image
                top = top + jnp.sum(c[xp] * f0[zp, yp, xp, 4:8], axis=0)
                bottom = bottom + jnp.sum(c[xp] * image, axis=0)
            numer = numer + jnp.where(mine, top, 0.0)
            denom = denom + jnp.where(mine, bottom, 0.0)
    lower = lanes((8, 128)) < 64
    both = jnp.where(lower, numer + pltpu.roll(numer, 64, 1), denom + pltpu.roll(denom, 64, 1))
    part = jnp.sum(both, axis=0, keepdims=True)
    sb[0] = part
    first_copies = []
    for k, (c, z) in enumerate(first_group):
        copy = remote(sb.at[0], ar1.at[k], s1.at[k], r1.at[k], along_z(c, z))
        copy.start()
        first_copies.append(copy)

    for zp in range(2):
        for yp in range(2):
            for xp in range(2):
                for i in range(4):
                    rows = window(zp, yp, 4 + i)[1]
                    stage[0, xp, rows, :] = v0[zp, yp, xp, 4 + i]
                    stage[1, xp, rows, :] = images[zp, yp, xp][i]
    for t, target in enumerate((prec, imag)):
        block = jnp.concatenate([stage[t, 0, 24:88, :], stage[t, 1, 24:88, :]], axis=1)
        target[...] = permuted(block, merge).reshape(8, 8, 256)
    out_copies = [
        pltpu.make_async_copy(prec, prec_hbm, io.at[1]),
        pltpu.make_async_copy(imag, imag_hbm, io.at[2]),
    ]
    for copy in out_copies:
        copy.start()

    for copy in first_copies:
        copy.wait_recv()
    part = part + jnp.sum(ar1[...], axis=0)
    sb[1] = part
    second_copies = []
    for k, (x, y) in enumerate(second_group):
        copy = remote(sb.at[1], ar2.at[k], s2.at[k], r2.at[k], along_xy(x, y))
        copy.start()
        second_copies.append(copy)
    for copy in second_copies:
        copy.wait_recv()
    part = part + jnp.sum(ar2[...], axis=0)
    left = lanes((1, 128)) < 64
    total_n = jnp.sum(jnp.where(left, part, 0.0), axis=1, keepdims=True)
    total_d = jnp.sum(jnp.where(left, 0.0, part), axis=1, keepdims=True)
    alpha_ref[...] = total_n / total_d
    for copy in out_copies:
        copy.wait()
    for copy in rhs_copies + field_copies + coarse_copies + first_copies + second_copies:
        copy.wait_send()


def solution(mesh):
    ngz, ngy = mesh.shape["gz"], mesh.shape["gy"]
    nz = ngz // (NX_CHIPS * CORES)
    coarse = 4 * ngy - 1
    one = nz * CORES - 1
    two = NX_CHIPS * ngy - 1

    def body(right_side):
        out = jax.ShapeDtypeStruct(right_side.shape, F32)
        vm = pltpu.VMEM
        dma = pltpu.SemaphoreType.DMA
        precond, image, alpha = pl.pallas_call(
            functools.partial(kernel, ngz, ngy),
            name="cg_iteration",
            out_shape=(pltpu.VMEM(right_side.shape, F32), pltpu.VMEM(right_side.shape, F32), jax.ShapeDtypeStruct((1, 1), F32)),
            in_specs=[pl.BlockSpec(memory_space=pltpu.HBM)],
            out_specs=(
                pl.BlockSpec(memory_space=pl.ANY),
                pl.BlockSpec(memory_space=pl.ANY),
                pl.BlockSpec(memory_space=pltpu.VMEM),
            ),
            scratch_shapes=[
                vm((8, 8, 256), F32),
                vm((2, 64, 128), F32),
                vm((3, 2, 128, 128), F32),
                vm((2, 2, 2, 12, 8, 128), F32),
                vm((2, 2, 2, 12, 8, 128), F32),
                vm((2, 2, 2, 12, 8, 128), F32),
                vm((2, 12, 8, 128), F32),
                vm((2, 128, 128), F32),
                vm((3, 2, 128, 128), F32),
                vm((32, 128), F32),
                vm((ngy, 64, 128), F32),
                vm((2, 2, 2 * ngy, 8, 128), F32),
                vm((2, 2, 2 * ngy + 2, 8, 128), F32),
                vm((2, 2, 2 * ngy + 2, 8, 128), F32),
                vm((2, ngy, 8, 128), F32),
                vm((2, ngy + 2, 8, 128), F32),
                vm((4, 16, 128), F32),
                vm((2, 2, 128, 128), F32),
                vm((8, 8, 256), F32),
                vm((8, 8, 256), F32),
                vm((2, 1, 128), F32),
                vm((one, 1, 128), F32),
                vm((two, 1, 128), F32),
                pltpu.SemaphoreType.REGULAR, pltpu.SemaphoreType.REGULAR((2,)), pltpu.SemaphoreType.REGULAR,
                dma((3,)), dma((8,)), dma((8,)), dma((8,)), dma((8,)), dma((coarse,)), dma((coarse,)),
                dma((one,)), dma((one,)), dma((two,)), dma((two,)),
            ],
            compiler_params=pltpu.CompilerParams(collective_id=0, has_side_effects=True, vmem_limit_bytes=60000000),
        )(right_side)
        return alpha[:, :, None] * precond, right_side - alpha[:, :, None] * image

    return jax.shard_map(
        body,
        mesh=mesh,
        in_specs=(P("gz", "gy", None),),
        out_specs=(P("gz", "gy", None), P("gz", "gy", None)),
        check_vma=False,
    )
```

```python
import functools

import jax
import jax.numpy as jnp
from jax import lax
from jax.experimental import pallas as pl
from jax.experimental.pallas import tpu as pltpu
from jax.sharding import PartitionSpec as P

MESH = pl.DeviceIdType.MESH
F32 = jnp.float32
INV = 1.0 / 26.0
NX_CHIPS = 4
CORES = 2

SWEEP = [
    ((0, 0), (0, 1)),
    ((0, 1), (0, 1)),
    ((1, 0), (0, 1)),
    ((1, 1), (0, 1, 0)),
    ((1, 0), (1, 0)),
    ((0, 1), (1, 0)),
    ((0, 0), (1, 0)),
]
PRE_ROWS = [(1, 11), (1, 10), (2, 10), (2, 9), (3, 9), (3, 8), (4, 8)]
POST_ROWS = [(1, 12), (1, 11), (2, 11), (2, 10), (3, 10), (3, 9), (4, 9)]


def lanes(shape):
    return lax.broadcasted_iota(jnp.int32, shape, len(shape) - 1)


def sublanes(shape):
    return lax.broadcasted_iota(jnp.int32, shape, len(shape) - 2)


def from_left(u, step=1):
    return jnp.where(lanes(u.shape) >= step, pltpu.roll(u, step, u.ndim - 1), 0.0)


def from_right(u, step=1):
    return jnp.where(lanes(u.shape) < 128 - step, pltpu.roll(u, 128 - step, u.ndim - 1), 0.0)


def both_sides(u, step=1):
    return from_left(u, step) + from_right(u, step)


def two_colours(base, f_sides, u, scale, step):
    sides = both_sides(u, step)
    place = lanes(u.shape)
    own = jnp.where(place >= step, u, 0.0) + jnp.where(place < 128 - step, u, 0.0)
    twice = both_sides(u, 2 * step) + own
    first = base + sides
    return first * scale, (first + (sides + f_sides + twice) * scale) * scale


def down(u):
    return pltpu.roll(u, 1, u.ndim - 2)


def up(u):
    return pltpu.roll(u, 7, u.ndim - 2)


def remote(src, dst, send, recv, where):
    copy = pltpu.make_async_remote_copy(
        src_ref=src, dst_ref=dst, send_sem=send, recv_sem=recv, device_id=where, device_id_type=MESH
    )
    return copy


def kernel(
    ngz, ngy, r_hbm, prec_hbm, imag_hbm, alpha_ref,
    rin, ownr, rd, g0, g1, g2, f0, v0, p0, mk, own, fw, dcb, dall, f1, v1, p1, f2, v2, vc, stage, prec, imag, sb, ar1, ar2,
    near, far, beside, io, rs, rr, fs, fr, cs, cr, s1, r1, s2, r2,
):
    gz = lax.axis_index("gz")
    gy = lax.axis_index("gy")
    nz = ngz // (NX_CHIPS * CORES)
    core = lax.rem(gz, CORES)
    chip_x = lax.rem(gz // CORES, NX_CHIPS)
    chip_z = gz // (CORES * NX_CHIPS)

    def at(dz, dy):
        return (lax.rem(gz + dz % ngz, ngz), lax.rem(gy + dy % ngy, ngy))

    def along_z(dc, dz):
        z = lax.rem(chip_z + dz % nz, nz)
        return ((z * NX_CHIPS + chip_x) * CORES + lax.rem(core + dc % CORES, CORES), gy)

    def along_xy(dx, dy):
        x = lax.rem(chip_x + dx % NX_CHIPS, NX_CHIPS)
        return ((chip_z * NX_CHIPS + x) * CORES + core, lax.rem(gy + dy % ngy, ngy))

    coarse_sends = [
        (slot, dz, dy)
        for dy in sorted(range(ngy), key=lambda d: (min(d, ngy - d) > 2, -min(d, ngy - d)))
        for slot, dz in ((2, 0), (1, 1), (3, -1), (0, 2))
        if not (dz == 0 and dy == 0)
    ]
    first_group = [(c, z) for z in range(nz) for c in range(CORES) if (c, z) != (0, 0)]
    first_group.sort(key=lambda g: -min(g[1], nz - g[1]))
    second_group = [(x, y) for y in range(ngy) for x in range(NX_CHIPS) if (x, y) != (0, 0)]
    second_group.sort(key=lambda g: -min(g[1], ngy - g[1]) - min(g[0], NX_CHIPS - g[0]))
    halo = [(dz, dy) for dz in (0, 1, -1) for dy in (0, 1, -1) if (dz, dy) != (0, 0)]

    load = pltpu.make_async_copy(r_hbm, rin, io.at[0])
    load.start()

    barrier = pltpu.get_barrier_semaphore()
    greeted = [at(dz, dy) for dz, dy in halo]
    greeted += [along_z(0, z) for z in (1, -1, 2, -2) if z % nz]
    greeted += [along_xy(x, 0) for x in range(1, NX_CHIPS)]

    def tell(semaphore, devices):
        for device in devices:
            pl.semaphore_signal(semaphore, inc=1, device_id=device, device_id_type=MESH)

    tell(barrier, greeted)
    two_away = [along_z(0, z) for z in (2, -2) if z % nz]
    three_away = [along_z(0, z) for z in (3, -3) if z % nz]

    row = lax.broadcasted_iota(jnp.int32, (256, 256), 0)
    col = lax.broadcasted_iota(jnp.int32, (256, 256), 1)
    split = (row == jnp.where(col < 128, 2 * col, 2 * col - 255)).astype(F32).astype(jnp.bfloat16)
    merge = (col == jnp.where(row < 128, 2 * row, 2 * row - 255)).astype(F32).astype(jnp.bfloat16)

    def permuted(block, matrix):
        high = block.astype(jnp.bfloat16)
        rest = block - high.astype(F32)
        middle = rest.astype(jnp.bfloat16)
        low = (rest - middle.astype(F32)).astype(jnp.bfloat16)
        moved = [
            lax.dot_general(part, matrix, (((1,), (0,)), ((), ())), preferred_element_type=F32)
            for part in (high, middle, low)
        ]
        return (moved[0] + moved[1]) + moved[2]

    for yb in range(3):
        rd[yb, :, 0:8, :] = jnp.zeros((2, 8, 128), F32)
        rd[yb, :, 112:128, :] = jnp.zeros((2, 16, 128), F32)
        fw[yb, :, 120:128, :] = jnp.zeros((2, 8, 128), F32)
    fw[1, :, 24:88, :] = jnp.zeros((2, 64, 128), F32)
    dall[:, 0:8, :] = jnp.zeros((ngy, 8, 128), F32)
    v0[...] = jnp.zeros(v0.shape, F32)
    p0[...] = jnp.zeros(p0.shape, F32)
    v1[...] = jnp.zeros(v1.shape, F32)
    p1[...] = jnp.zeros(p1.shape, F32)
    v2[...] = jnp.zeros(v2.shape, F32)

    load.wait()
    both = permuted(rin[...].reshape(64, 256), split)
    for xp in range(2):
        part = both[:, 128 * xp : 128 * xp + 128]
        ownr[xp] = part
        rd[1, xp, 24:88, :] = part

    sub = sublanes((8, 128))
    for zp in range(2):
        z = gz * 8 + 2 * sub - (2 + zp)
        z_in = ((z >= 0) & (z < ngz * 8)).astype(F32)
        low = jnp.where(gy > 0, 1.0, 0.0).astype(F32)
        high = jnp.where(gy < ngy - 1, 1.0, 0.0).astype(F32)
        mk[zp, 0:4] = jnp.broadcast_to(z_in * low, (4, 8, 128))
        mk[zp, 4:8] = jnp.broadcast_to(z_in, (4, 8, 128))
        mk[zp, 8:12] = jnp.broadcast_to(z_in * high, (4, 8, 128))

    def own_rows(zp, shape):
        s = sublanes(shape)
        return (s >= 1 + zp) & (s < 5 + zp)

    pl.semaphore_wait(barrier, len(greeted))

    def border(source, target, rows, sends, arrivals):
        copies = []
        for k, (dz, dy) in enumerate(halo):
            z_from, count, z_to = rows[dz]
            copy = remote(
                source.at[:, pl.ds(8 * z_from, 8 * count), :],
                target.at[1 - dy, :, pl.ds(8 * z_to, 8 * count), :],
                sends.at[k], arrivals.at[k], at(dz, dy),
            )
            copy.start()
            copies.append(copy)
        return copies

    tell(far.at[0], two_away)
    rhs_copies = border(ownr, rd, {0: (0, 8, 3), 1: (6, 2, 1), -1: (0, 3, 11)}, rs, rr)
    for copy in rhs_copies:
        copy.wait_recv()
    tell(near, [at(0, 2), at(0, -2)])
    if two_away:
        pl.semaphore_wait(far.at[0], len(two_away))
    tell(far.at[1], three_away)

    def window(zp, yp, i):
        return i // 4, pl.ds(8 * (1 - zp) + 2 * (i % 4) + yp, 8, stride=16)

    for zp in range(2):
        for yp in range(2):
            for xp in range(2):
                for i in range(12):
                    yb, rows = window(zp, yp, i)
                    value = rd[yb, xp, rows, :]
                    f0[zp, yp, xp, i] = value
                    g0[zp, yp, xp, i] = value + (from_right(value) if xp == 0 else from_left(value))

    def pair0(zp, c):
        return c + (down(c) if zp == 0 else up(c))

    def outer0(zp, yp, lo, hi):
        a = -1 if yp == 0 else 0
        sums = []
        for xp in range(2):
            s = v0[zp, 1 - yp, xp, lo + a : hi + a] + v0[zp, 1 - yp, xp, lo + a + 1 : hi + a + 1]
            q = p0[1 - zp, 1 - yp, xp, lo + a : hi + a] + p0[1 - zp, 1 - yp, xp, lo + a + 1 : hi + a + 1]
            sums.append(s + q + p0[1 - zp, yp, xp, lo:hi])
        return sums

    def beside0(u, xp):
        return u + (from_left(u) if xp == 0 else from_right(u))

    def around0(s, c, xp):
        return s[xp] + beside0(s[1 - xp] + c[1 - xp], xp)

    def phase0(group, order, lo, hi):
        zp, yp = group
        s = outer0(zp, yp, lo, hi)
        c = [v0[zp, yp, 0, lo:hi], v0[zp, yp, 1, lo:hi]]
        scale = mk[zp, lo:hi] * INV
        f = [f0[zp, yp, 0, lo:hi], f0[zp, yp, 1, lo:hi]]
        a, b = order[:2]
        u = s[b] + c[b]
        left, right = from_left(u), from_right(u)
        edge = lanes(u.shape) < 127 if a == 0 else lanes(u.shape) >= 1
        twice = u + left + right + jnp.where(edge, u, 0.0)
        cross = beside0(s[a], b)
        c[a] = (s[a] + f[a] + (u + (left if a == 0 else right))) * scale
        c[b] = (s[b] + f[b] + cross + (cross + g0[zp, yp, a, lo:hi] + twice) * scale) * scale
        for xp in order[2:]:
            c[xp] = (around0(s, c, xp) + f[xp]) * scale
        for xp in range(2):
            v0[zp, yp, xp, lo:hi] = c[xp]
            p0[zp, yp, xp, lo:hi] = pair0(zp, c[xp])

    for (group, order), (lo, hi) in zip(SWEEP, PRE_ROWS):
        phase0(group, order, lo, hi)

    s = outer0(0, 0, 4, 8)
    c = [v0[0, 0, 0, 4:8], v0[0, 0, 1, 4:8]]
    defect = up(f0[0, 0, 0, 4:8] - (26.0 * c[0] - around0(s, c, 0)))
    for i in range(4):
        dcb[pl.ds(i, 8, stride=4), :] = defect[i]
    for zp in range(2):
        for yp in range(2):
            for xp in range(2):
                for i in range(4, 8):
                    own[xp, window(zp, yp, i)[1], :] = v0[zp, yp, xp, i]
    coarse_copies = []
    reached = sum(min(dy, ngy - dy) <= 2 for _, _, dy in coarse_sends) % len(coarse_sends)
    for k, (slot, dz, dy) in enumerate(coarse_sends):
        if k == reached:
            pl.semaphore_wait(near, 2)
        first, count = (8, 8) if slot == 0 else (0, 16)
        copy = remote(
            dcb.at[pl.ds(first, count), :], dall.at[gy, pl.ds(16 * slot + first, count), :],
            cs.at[k], cr.at[k], at(dz, dy),
        )
        copy.start()
        coarse_copies.append(copy)
    field_copies = border(own, fw, {0: (3, 8, 3), 1: (8, 3, 0), -1: (3, 4, 11)}, fs, fr)
    dall[gy, 32:48, :] = dcb[0:16, :]

    for copy in coarse_copies:
        copy.wait_recv()
    if three_away:
        pl.semaphore_wait(far.at[1], len(three_away))
    tell(beside, [along_z(1, 0)])

    n1 = 2 * ngy
    for zp in range(2):
        for yp in range(2):
            for i in range(n1):
                value = dall[i // 2, pl.ds(2 * (i % 2) + yp + 4 * zp, 8, stride=8), :]
                f1[zp, yp, i] = value
                g1[zp, yp, i] = both_sides(value)

    scale1 = []
    for zp in range(2):
        z = gz * 4 + 2 * sub - (8 - zp)
        scale1.append(jnp.where((z >= 0) & (z < ngz * 4), INV, 0.0).astype(F32)[None])

    def pair1(zp, c):
        return c + (up(c) if zp == 0 else down(c))

    def outer1(zp, yp):
        a = 0 if yp == 0 else 1
        s = v1[zp, 1 - yp, a : a + n1] + v1[zp, 1 - yp, a + 1 : a + 1 + n1]
        q = p1[1 - zp, 1 - yp, a : a + n1] + p1[1 - zp, 1 - yp, a + 1 : a + 1 + n1]
        return s + q + p1[1 - zp, yp, 1 : 1 + n1]

    def phase1(group, order):
        zp, yp = group
        s = outer1(zp, yp)
        c = v1[zp, yp, 1 : 1 + n1]
        base = s + f1[zp, yp]
        parity = lax.rem(lanes(c.shape), 2)
        u = s + jnp.where(parity == order[1], c, 0.0)
        first, second = two_colours(base, g1[zp, yp], u, scale1[zp], 1)
        c = jnp.where(parity == order[0], first, second)
        for xp in order[2:]:
            c = jnp.where(parity == xp, (base + both_sides(s + c)) * scale1[zp], c)
        v1[zp, yp, 1 : 1 + n1] = c
        p1[zp, yp, 1 : 1 + n1] = pair1(zp, c)

    for group, order in SWEEP:
        phase1(group, order)

    n2 = ngy
    s = outer1(0, 0)
    c = v1[0, 0, 1 : 1 + n1]
    even = lax.rem(lanes(c.shape), 2) == 0
    defect = jnp.where(even, f1[0, 0] - (26.0 * c - (s + both_sides(s + c))), 0.0)
    for i in range(n1):
        f2[i % 2, i // 2] = defect[i]
        g2[i % 2, i // 2] = both_sides(defect[i], 2)
    z = gz * 2 + sub - 4
    scale2 = jnp.where((z >= 0) & (z < ngz * 2), INV, 0.0).astype(F32)[None]

    for group, order in SWEEP:
        zp, yp = group
        a = 0 if yp == 0 else 1
        c = v2[yp, 1 : 1 + n2]
        side = v2[1 - yp, a : a + n2] + v2[1 - yp, a + 1 : a + 1 + n2]
        column = side + c
        s = side + (down(column) + up(column))
        base = s + f2[yp]
        layer = lax.rem(sublanes(c.shape), 2) == zp
        place = lax.rem(lanes(c.shape), 4)
        u = s + jnp.where(place == 2 * order[1], c, 0.0)
        first, second = two_colours(base, g2[yp], u, scale2, 2)
        c = jnp.where(layer & (place == 2 * order[0]), first, jnp.where(layer & (place == 2 * order[1]), second, c))
        for xp in order[2:]:
            c = jnp.where(layer & (place == 2 * xp), (base + both_sides(s + c, 2)) * scale2, c)
        v2[yp, 1 : 1 + n2] = c

    held = sublanes((8, 128))
    mine = (held >= 4) & (held < 6)
    for i in range(n1):
        value = v1[0, 0, 1 + i] + jnp.where(mine, v2[i % 2, 1 + i // 2], 0.0)
        v1[0, 0, 1 + i] = value
        p1[0, 0, 1 + i] = pair1(0, value)
    for group, order in SWEEP:
        phase1(group, order)

    pl.semaphore_wait(beside, 1)

    for i in range(4):
        for zp in range(2):
            vc[i, pl.ds(zp, 8, stride=2), :] = v1[zp, i % 2, 1 + 2 * gy + i // 2]
    for copy in field_copies:
        copy.wait_recv()
    for zp in range(2):
        for yp in range(2):
            for xp in range(2):
                for i in range(12):
                    yb, rows = window(zp, yp, i)
                    value = fw[yb, xp, rows, :] * mk[zp, i]
                    if yb == 1:
                        value = jnp.where(own_rows(zp, (8, 128)), v0[zp, yp, xp, i], value)
                    v0[zp, yp, xp, i] = value
                    if zp == 1:
                        p0[zp, yp, xp, i] = pair0(zp, value)
    for i in range(4):
        v0[0, 0, 0, 4 + i] += jnp.where(own_rows(0, (8, 128)), vc[i, 7:15, :], 0.0)

    for (group, order), (lo, hi) in zip(SWEEP, POST_ROWS):
        phase0(group, order, lo, hi)

    numer = jnp.zeros((8, 128), F32)
    denom = jnp.zeros((8, 128), F32)
    images = {}
    for zp in range(2):
        for yp in range(2):
            s = outer0(zp, yp, 4, 8)
            c = [v0[zp, yp, 0, 4:8], v0[zp, yp, 1, 4:8]]
            mine = own_rows(zp, (8, 128))
            top, bottom = 0.0, 0.0
            for xp in range(2):
                image = 26.0 * c[xp] - around0(s, c, xp)
                images[zp, yp, xp] = image
                top = top + jnp.sum(c[xp] * f0[zp, yp, xp, 4:8], axis=0)
                bottom = bottom + jnp.sum(c[xp] * image, axis=0)
            numer = numer + jnp.where(mine, top, 0.0)
            denom = denom + jnp.where(mine, bottom, 0.0)
    lower = lanes((8, 128)) < 64
    both = jnp.where(lower, numer + pltpu.roll(numer, 64, 1), denom + pltpu.roll(denom, 64, 1))
    part = jnp.sum(both, axis=0, keepdims=True)
    sb[0] = part
    first_copies = []
    for k, (c, z) in enumerate(first_group):
        copy = remote(sb.at[0], ar1.at[k], s1.at[k], r1.at[k], along_z(c, z))
        copy.start()
        first_copies.append(copy)

    for zp in range(2):
        for yp in range(2):
            for xp in range(2):
                for i in range(4):
                    rows = window(zp, yp, 4 + i)[1]
                    stage[0, xp, rows, :] = v0[zp, yp, xp, 4 + i]
                    stage[1, xp, rows, :] = images[zp, yp, xp][i]
    for t, target in enumerate((prec, imag)):
        block = jnp.concatenate([stage[t, 0, 24:88, :], stage[t, 1, 24:88, :]], axis=1)
        target[...] = permuted(block, merge).reshape(8, 8, 256)
    out_copies = [
        pltpu.make_async_copy(prec, prec_hbm, io.at[1]),
        pltpu.make_async_copy(imag, imag_hbm, io.at[2]),
    ]
    for copy in out_copies:
        copy.start()

    for copy in first_copies:
        copy.wait_recv()
    part = part + jnp.sum(ar1[...], axis=0)
    sb[1] = part
    second_copies = []
    for k, (x, y) in enumerate(second_group):
        copy = remote(sb.at[1], ar2.at[k], s2.at[k], r2.at[k], along_xy(x, y))
        copy.start()
        second_copies.append(copy)
    for copy in second_copies:
        copy.wait_recv()
    part = part + jnp.sum(ar2[...], axis=0)
    left = lanes((1, 128)) < 64
    total_n = jnp.sum(jnp.where(left, part, 0.0), axis=1, keepdims=True)
    total_d = jnp.sum(jnp.where(left, 0.0, part), axis=1, keepdims=True)
    alpha_ref[...] = total_n / total_d
    for copy in out_copies:
        copy.wait()
    for copy in rhs_copies + field_copies + coarse_copies + first_copies + second_copies:
        copy.wait_send()


def solution(mesh):
    ngz, ngy = mesh.shape["gz"], mesh.shape["gy"]
    nz = ngz // (NX_CHIPS * CORES)
    coarse = 4 * ngy - 1
    one = nz * CORES - 1
    two = NX_CHIPS * ngy - 1

    def body(right_side):
        out = jax.ShapeDtypeStruct(right_side.shape, F32)
        vm = pltpu.VMEM
        dma = pltpu.SemaphoreType.DMA
        precond, image, alpha = pl.pallas_call(
            functools.partial(kernel, ngz, ngy),
            name="cg_iteration",
            out_shape=(pltpu.VMEM(right_side.shape, F32), pltpu.VMEM(right_side.shape, F32), jax.ShapeDtypeStruct((1, 1), F32)),
            in_specs=[pl.BlockSpec(memory_space=pltpu.HBM)],
            out_specs=(
                pl.BlockSpec(memory_space=pl.ANY),
                pl.BlockSpec(memory_space=pl.ANY),
                pl.BlockSpec(memory_space=pltpu.VMEM),
            ),
            scratch_shapes=[
                vm((8, 8, 256), F32),
                vm((2, 64, 128), F32),
                vm((3, 2, 128, 128), F32),
                vm((2, 2, 2, 12, 8, 128), F32),
                vm((2, 2, 2 * ngy, 8, 128), F32),
                vm((2, ngy, 8, 128), F32),
                vm((2, 2, 2, 12, 8, 128), F32),
                vm((2, 2, 2, 12, 8, 128), F32),
                vm((2, 2, 2, 12, 8, 128), F32),
                vm((2, 12, 8, 128), F32),
                vm((2, 128, 128), F32),
                vm((3, 2, 128, 128), F32),
                vm((32, 128), F32),
                vm((ngy, 64, 128), F32),
                vm((2, 2, 2 * ngy, 8, 128), F32),
                vm((2, 2, 2 * ngy + 2, 8, 128), F32),
                vm((2, 2, 2 * ngy + 2, 8, 128), F32),
                vm((2, ngy, 8, 128), F32),
                vm((2, ngy + 2, 8, 128), F32),
                vm((4, 16, 128), F32),
                vm((2, 2, 128, 128), F32),
                vm((8, 8, 256), F32),
                vm((8, 8, 256), F32),
                vm((2, 1, 128), F32),
                vm((one, 1, 128), F32),
                vm((two, 1, 128), F32),
                pltpu.SemaphoreType.REGULAR, pltpu.SemaphoreType.REGULAR((2,)), pltpu.SemaphoreType.REGULAR,
                dma((3,)), dma((8,)), dma((8,)), dma((8,)), dma((8,)), dma((coarse,)), dma((coarse,)),
                dma((one,)), dma((one,)), dma((two,)), dma((two,)),
            ],
            compiler_params=pltpu.CompilerParams(collective_id=0, has_side_effects=True, vmem_limit_bytes=60000000),
        )(right_side)
        return alpha[:, :, None] * precond, right_side - alpha[:, :, None] * image

    return jax.shard_map(
        body,
        mesh=mesh,
        in_specs=(P("gz", "gy", None),),
        out_specs=(P("gz", "gy", None), P("gz", "gy", None)),
        check_vma=False,
    )
```

```python
import functools

import jax
import jax.numpy as jnp
from jax import lax
from jax.experimental import pallas as pl
from jax.experimental.pallas import tpu as pltpu
from jax.sharding import PartitionSpec as P

MESH = pl.DeviceIdType.MESH
F32 = jnp.float32
INV = 1.0 / 26.0
NX_CHIPS = 4
CORES = 2

SWEEP = [
    ((0, 0), (0, 1)),
    ((0, 1), (0, 1)),
    ((1, 0), (0, 1)),
    ((1, 1), (0, 1, 0)),
    ((1, 0), (1, 0)),
    ((0, 1), (1, 0)),
    ((0, 0), (1, 0)),
]
PRE_ROWS = [(1, 11), (1, 10), (2, 10), (2, 9), (3, 9), (3, 8), (4, 8)]
POST_ROWS = [(1, 12), (1, 11), (2, 11), (2, 10), (3, 10), (3, 9), (4, 9)]


def lanes(shape):
    return lax.broadcasted_iota(jnp.int32, shape, len(shape) - 1)


def sublanes(shape):
    return lax.broadcasted_iota(jnp.int32, shape, len(shape) - 2)


def from_left(u, step=1):
    return jnp.where(lanes(u.shape) >= step, pltpu.roll(u, step, u.ndim - 1), 0.0)


def from_right(u, step=1):
    return jnp.where(lanes(u.shape) < 128 - step, pltpu.roll(u, 128 - step, u.ndim - 1), 0.0)


def both_sides(u, step=1):
    return from_left(u, step) + from_right(u, step)


def two_colours(base, f_sides, u, scale, step):
    sides = both_sides(u, step)
    place = lanes(u.shape)
    own = jnp.where(place >= step, u, 0.0) + jnp.where(place < 128 - step, u, 0.0)
    twice = both_sides(u, 2 * step) + own
    first = base + sides
    return first * scale, (first + (sides + f_sides + twice) * scale) * scale


def down(u):
    return pltpu.roll(u, 1, u.ndim - 2)


def up(u):
    return pltpu.roll(u, 7, u.ndim - 2)


def remote(src, dst, send, recv, where):
    copy = pltpu.make_async_remote_copy(
        src_ref=src, dst_ref=dst, send_sem=send, recv_sem=recv, device_id=where, device_id_type=MESH
    )
    return copy


def kernel(
    ngz, ngy, r_hbm, prec_hbm, imag_hbm, alpha_ref,
    rin, ownr, rd, g0, g1, g2, f0, v0, p0, mk, own, fw, dcb, dall, f1, v1, p1, f2, v2, vc, stage, prec, imag, sb, ar1, ar2,
    near, far, beside, io, rs, rr, fs, fr, cs, cr, s1, r1, s2, r2,
):
    gz = lax.axis_index("gz")
    gy = lax.axis_index("gy")
    nz = ngz // (NX_CHIPS * CORES)
    core = lax.rem(gz, CORES)
    chip_x = lax.rem(gz // CORES, NX_CHIPS)
    chip_z = gz // (CORES * NX_CHIPS)

    def at(dz, dy):
        return (lax.rem(gz + dz % ngz, ngz), lax.rem(gy + dy % ngy, ngy))

    def along_z(dc, dz):
        z = lax.rem(chip_z + dz % nz, nz)
        return ((z * NX_CHIPS + chip_x) * CORES + lax.rem(core + dc % CORES, CORES), gy)

    def along_xy(dx, dy):
        x = lax.rem(chip_x + dx % NX_CHIPS, NX_CHIPS)
        return ((chip_z * NX_CHIPS + x) * CORES + core, lax.rem(gy + dy % ngy, ngy))

    coarse_sends = [
        (slot, dz, dy)
        for dy in sorted(range(ngy), key=lambda d: (min(d, ngy - d) > 2, -min(d, ngy - d)))
        for slot, dz in ((2, 0), (1, 1), (3, -1), (0, 2))
        if not (dz == 0 and dy == 0)
    ]
    first_group = [(c, z) for z in range(nz) for c in range(CORES) if (c, z) != (0, 0)]
    first_group.sort(key=lambda g: -min(g[1], nz - g[1]))
    second_group = [(x, y) for y in range(ngy) for x in range(NX_CHIPS) if (x, y) != (0, 0)]
    second_group.sort(key=lambda g: -min(g[1], ngy - g[1]) - min(g[0], NX_CHIPS - g[0]))
    halo = [(dz, dy) for dz in (0, 1, -1) for dy in (0, 1, -1) if (dz, dy) != (0, 0)]

    load = pltpu.make_async_copy(r_hbm, rin, io.at[0])
    load.start()

    barrier = pltpu.get_barrier_semaphore()
    greeted = [at(dz, dy) for dz, dy in halo]
    greeted += [along_z(0, z) for z in (1, -1, 2, -2) if z % nz]
    greeted += [along_xy(x, 0) for x in range(1, NX_CHIPS)]

    def tell(semaphore, devices):
        for device in devices:
            pl.semaphore_signal(semaphore, inc=1, device_id=device, device_id_type=MESH)

    tell(barrier, greeted)
    two_away = [along_z(0, z) for z in (2, -2) if z % nz]
    three_away = [along_z(0, z) for z in (3, -3) if z % nz]

    row = lax.broadcasted_iota(jnp.int32, (256, 256), 0)
    col = lax.broadcasted_iota(jnp.int32, (256, 256), 1)
    split = (row == jnp.where(col < 128, 2 * col, 2 * col - 255)).astype(F32).astype(jnp.bfloat16)
    merge = (col == jnp.where(row < 128, 2 * row, 2 * row - 255)).astype(F32).astype(jnp.bfloat16)

    def permuted(block, matrix):
        high = block.astype(jnp.bfloat16)
        rest = block - high.astype(F32)
        middle = rest.astype(jnp.bfloat16)
        low = (rest - middle.astype(F32)).astype(jnp.bfloat16)
        moved = [
            lax.dot_general(part, matrix, (((1,), (0,)), ((), ())), preferred_element_type=F32)
            for part in (high, middle, low)
        ]
        return (moved[0] + moved[1]) + moved[2]

    for yb in range(3):
        rd[yb, :, 0:8, :] = jnp.zeros((2, 8, 128), F32)
        rd[yb, :, 112:128, :] = jnp.zeros((2, 16, 128), F32)
        fw[yb, :, 120:128, :] = jnp.zeros((2, 8, 128), F32)
    fw[1, :, 24:88, :] = jnp.zeros((2, 64, 128), F32)
    dall[:, 0:8, :] = jnp.zeros((ngy, 8, 128), F32)
    v0[...] = jnp.zeros(v0.shape, F32)
    p0[...] = jnp.zeros(p0.shape, F32)
    v1[...] = jnp.zeros(v1.shape, F32)
    p1[...] = jnp.zeros(p1.shape, F32)
    v2[...] = jnp.zeros(v2.shape, F32)

    load.wait()
    both = permuted(rin[...].reshape(64, 256), split)
    for xp in range(2):
        part = both[:, 128 * xp : 128 * xp + 128]
        ownr[xp] = part
        rd[1, xp, 24:88, :] = part

    sub = sublanes((8, 128))
    for zp in range(2):
        z = gz * 8 + 2 * sub - (2 + zp)
        z_in = ((z >= 0) & (z < ngz * 8)).astype(F32)
        low = jnp.where(gy > 0, 1.0, 0.0).astype(F32)
        high = jnp.where(gy < ngy - 1, 1.0, 0.0).astype(F32)
        mk[zp, 0:4] = jnp.broadcast_to(z_in * low, (4, 8, 128))
        mk[zp, 4:8] = jnp.broadcast_to(z_in, (4, 8, 128))
        mk[zp, 8:12] = jnp.broadcast_to(z_in * high, (4, 8, 128))

    def own_rows(zp, shape):
        s = sublanes(shape)
        return (s >= 1 + zp) & (s < 5 + zp)

    pl.semaphore_wait(barrier, len(greeted))

    def border(source, target, rows, sends, arrivals):
        copies = []
        for k, (dz, dy) in enumerate(halo):
            z_from, count, z_to = rows[dz]
            copy = remote(
                source.at[:, pl.ds(8 * z_from, 8 * count), :],
                target.at[1 - dy, :, pl.ds(8 * z_to, 8 * count), :],
                sends.at[k], arrivals.at[k], at(dz, dy),
            )
            copy.start()
            copies.append(copy)
        return copies

    tell(far.at[0], two_away)
    rhs_copies = border(ownr, rd, {0: (0, 8, 3), 1: (6, 2, 1), -1: (0, 3, 11)}, rs, rr)
    for copy in rhs_copies:
        copy.wait_recv()
    tell(near, [at(0, 2), at(0, -2)])
    if two_away:
        pl.semaphore_wait(far.at[0], len(two_away))
    tell(far.at[1], three_away)

    def window(zp, yp, i):
        return i // 4, pl.ds(8 * (1 - zp) + 2 * (i % 4) + yp, 8, stride=16)

    for zp in range(2):
        for yp in range(2):
            for xp in range(2):
                for i in range(12):
                    yb, rows = window(zp, yp, i)
                    value = rd[yb, xp, rows, :]
                    f0[zp, yp, xp, i] = value
                    g0[zp, yp, xp, i] = value + (from_right(value) if xp == 0 else from_left(value))

    def pair0(zp, c):
        return c + (down(c) if zp == 0 else up(c))

    def outer0(zp, yp, lo, hi):
        a = -1 if yp == 0 else 0
        sums = []
        for xp in range(2):
            s = v0[zp, 1 - yp, xp, lo + a : hi + a] + v0[zp, 1 - yp, xp, lo + a + 1 : hi + a + 1]
            q = p0[1 - zp, 1 - yp, xp, lo + a : hi + a] + p0[1 - zp, 1 - yp, xp, lo + a + 1 : hi + a + 1]
            sums.append(s + q + p0[1 - zp, yp, xp, lo:hi])
        return sums

    def beside0(u, xp):
        return u + (from_left(u) if xp == 0 else from_right(u))

    def around0(s, c, xp):
        return s[xp] + beside0(s[1 - xp] + c[1 - xp], xp)

    def phase0(group, order, lo, hi):
        zp, yp = group
        s = outer0(zp, yp, lo, hi)
        c = [v0[zp, yp, 0, lo:hi], v0[zp, yp, 1, lo:hi]]
        scale = mk[zp, lo:hi] * INV
        f = [f0[zp, yp, 0, lo:hi], f0[zp, yp, 1, lo:hi]]
        a, b = order[:2]
        u = s[b] + c[b]
        left, right = from_left(u), from_right(u)
        edge = lanes(u.shape) < 127 if a == 0 else lanes(u.shape) >= 1
        twice = u + left + right + jnp.where(edge, u, 0.0)
        cross = beside0(s[a], b)
        c[a] = (s[a] + f[a] + (u + (left if a == 0 else right))) * scale
        c[b] = (s[b] + f[b] + cross + (cross + g0[zp, yp, a, lo:hi] + twice) * scale) * scale
        for xp in order[2:]:
            c[xp] = (around0(s, c, xp) + f[xp]) * scale
        for xp in range(2):
            v0[zp, yp, xp, lo:hi] = c[xp]
            p0[zp, yp, xp, lo:hi] = pair0(zp, c[xp])

    for (group, order), (lo, hi) in zip(SWEEP, PRE_ROWS):
        phase0(group, order, lo, hi)

    s = outer0(0, 0, 4, 8)
    c = [v0[0, 0, 0, 4:8], v0[0, 0, 1, 4:8]]
    defect = up(f0[0, 0, 0, 4:8] - (26.0 * c[0] - around0(s, c, 0)))
    for i in range(4):
        dcb[pl.ds(i, 8, stride=4), :] = defect[i]
    for zp in range(2):
        for yp in range(2):
            for xp in range(2):
                for i in range(4, 8):
                    own[xp, window(zp, yp, i)[1], :] = v0[zp, yp, xp, i]
    coarse_copies = []
    reached = sum(min(dy, ngy - dy) <= 2 for _, _, dy in coarse_sends) % len(coarse_sends)
    for k, (slot, dz, dy) in enumerate(coarse_sends):
        if k == reached:
            pl.semaphore_wait(near, 2)
        first, count = (8, 8) if slot == 0 else (0, 16)
        copy = remote(
            dcb.at[pl.ds(first, count), :], dall.at[gy, pl.ds(16 * slot + first, count), :],
            cs.at[k], cr.at[k], at(dz, dy),
        )
        copy.start()
        coarse_copies.append(copy)
    field_copies = border(own, fw, {0: (3, 8, 3), 1: (8, 3, 0), -1: (3, 4, 11)}, fs, fr)
    dall[gy, 32:48, :] = dcb[0:16, :]

    for copy in coarse_copies:
        copy.wait_recv()
    if three_away:
        pl.semaphore_wait(far.at[1], len(three_away))
    tell(beside, [along_z(1, 0)])

    n1 = 2 * ngy
    for zp in range(2):
        for yp in range(2):
            for i in range(n1):
                value = dall[i // 2, pl.ds(2 * (i % 2) + yp + 4 * zp, 8, stride=8), :]
                f1[zp, yp, i] = value
                g1[zp, yp, i] = both_sides(value)

    scale1 = []
    for zp in range(2):
        z = gz * 4 + 2 * sub - (8 - zp)
        scale1.append(jnp.where((z >= 0) & (z < ngz * 4), INV, 0.0).astype(F32)[None])

    def pair1(zp, c):
        return c + (up(c) if zp == 0 else down(c))

    def outer1(zp, yp):
        a = 0 if yp == 0 else 1
        s = v1[zp, 1 - yp, a : a + n1] + v1[zp, 1 - yp, a + 1 : a + 1 + n1]
        q = p1[1 - zp, 1 - yp, a : a + n1] + p1[1 - zp, 1 - yp, a + 1 : a + 1 + n1]
        return s + q + p1[1 - zp, yp, 1 : 1 + n1]

    def phase1(group, order):
        zp, yp = group
        s = outer1(zp, yp)
        c = v1[zp, yp, 1 : 1 + n1]
        base = s + f1[zp, yp]
        parity = lax.rem(lanes(c.shape), 2)
        u = s + jnp.where(parity == order[1], c, 0.0)
        first, second = two_colours(base, g1[zp, yp], u, scale1[zp], 1)
        c = jnp.where(parity == order[0], first, second)
        for xp in order[2:]:
            c = jnp.where(parity == xp, (base + both_sides(s + c)) * scale1[zp], c)
        v1[zp, yp, 1 : 1 + n1] = c
        p1[zp, yp, 1 : 1 + n1] = pair1(zp, c)

    for group, order in SWEEP:
        phase1(group, order)

    n2 = ngy
    s = outer1(0, 0)
    c = v1[0, 0, 1 : 1 + n1]
    even = lax.rem(lanes(c.shape), 2) == 0
    defect = jnp.where(even, f1[0, 0] - (26.0 * c - (s + both_sides(s + c))), 0.0)
    for i in range(n1):
        f2[i % 2, i // 2] = defect[i]
        g2[i % 2, i // 2] = both_sides(defect[i], 2)
    z = gz * 2 + sub - 4
    scale2 = jnp.where((z >= 0) & (z < ngz * 2), INV, 0.0).astype(F32)[None]

    for group, order in SWEEP:
        zp, yp = group
        a = 0 if yp == 0 else 1
        c = v2[yp, 1 : 1 + n2]
        side = v2[1 - yp, a : a + n2] + v2[1 - yp, a + 1 : a + 1 + n2]
        column = side + c
        s = side + (down(column) + up(column))
        base = s + f2[yp]
        layer = lax.rem(sublanes(c.shape), 2) == zp
        place = lax.rem(lanes(c.shape), 4)
        u = s + jnp.where(place == 2 * order[1], c, 0.0)
        first, second = two_colours(base, g2[yp], u, scale2, 2)
        c = jnp.where(layer & (place == 2 * order[0]), first, jnp.where(layer & (place == 2 * order[1]), second, c))
        for xp in order[2:]:
            c = jnp.where(layer & (place == 2 * xp), (base + both_sides(s + c, 2)) * scale2, c)
        v2[yp, 1 : 1 + n2] = c

    for copy in field_copies:
        copy.wait_recv()
    for zp in range(2):
        for yp in range(2):
            for xp in range(2):
                for i in range(12):
                    yb, rows = window(zp, yp, i)
                    value = fw[yb, xp, rows, :] * mk[zp, i]
                    if yb == 1:
                        value = jnp.where(own_rows(zp, (8, 128)), v0[zp, yp, xp, i], value)
                    v0[zp, yp, xp, i] = value
                    if zp == 1:
                        p0[zp, yp, xp, i] = pair0(zp, value)

    held = sublanes((8, 128))
    mine = (held >= 4) & (held < 6)
    for i in range(n1):
        value = v1[0, 0, 1 + i] + jnp.where(mine, v2[i % 2, 1 + i // 2], 0.0)
        v1[0, 0, 1 + i] = value
        p1[0, 0, 1 + i] = pair1(0, value)
    for group, order in SWEEP:
        phase1(group, order)

    pl.semaphore_wait(beside, 1)

    for i in range(4):
        for zp in range(2):
            vc[i, pl.ds(zp, 8, stride=2), :] = v1[zp, i % 2, 1 + 2 * gy + i // 2]
    for i in range(4):
        v0[0, 0, 0, 4 + i] += jnp.where(own_rows(0, (8, 128)), vc[i, 7:15, :], 0.0)

    for (group, order), (lo, hi) in zip(SWEEP, POST_ROWS):
        phase0(group, order, lo, hi)

    numer = jnp.zeros((8, 128), F32)
    denom = jnp.zeros((8, 128), F32)
    images = {}
    for zp in range(2):
        for yp in range(2):
            s = outer0(zp, yp, 4, 8)
            c = [v0[zp, yp, 0, 4:8], v0[zp, yp, 1, 4:8]]
            mine = own_rows(zp, (8, 128))
            top, bottom = 0.0, 0.0
            for xp in range(2):
                image = 26.0 * c[xp] - around0(s, c, xp)
                images[zp, yp, xp] = image
                top = top + jnp.sum(c[xp] * f0[zp, yp, xp, 4:8], axis=0)
                bottom = bottom + jnp.sum(c[xp] * image, axis=0)
            numer = numer + jnp.where(mine, top, 0.0)
            denom = denom + jnp.where(mine, bottom, 0.0)
    lower = lanes((8, 128)) < 64
    both = jnp.where(lower, numer + pltpu.roll(numer, 64, 1), denom + pltpu.roll(denom, 64, 1))
    part = jnp.sum(both, axis=0, keepdims=True)
    sb[0] = part
    first_copies = []
    for k, (c, z) in enumerate(first_group):
        copy = remote(sb.at[0], ar1.at[k], s1.at[k], r1.at[k], along_z(c, z))
        copy.start()
        first_copies.append(copy)

    for zp in range(2):
        for yp in range(2):
            for xp in range(2):
                for i in range(4):
                    rows = window(zp, yp, 4 + i)[1]
                    stage[0, xp, rows, :] = v0[zp, yp, xp, 4 + i]
                    stage[1, xp, rows, :] = images[zp, yp, xp][i]
    for t, target in enumerate((prec, imag)):
        block = jnp.concatenate([stage[t, 0, 24:88, :], stage[t, 1, 24:88, :]], axis=1)
        target[...] = permuted(block, merge).reshape(8, 8, 256)
    out_copies = [
        pltpu.make_async_copy(prec, prec_hbm, io.at[1]),
        pltpu.make_async_copy(imag, imag_hbm, io.at[2]),
    ]
    for copy in out_copies:
        copy.start()

    for copy in first_copies:
        copy.wait_recv()
    part = part + jnp.sum(ar1[...], axis=0)
    sb[1] = part
    second_copies = []
    for k, (x, y) in enumerate(second_group):
        copy = remote(sb.at[1], ar2.at[k], s2.at[k], r2.at[k], along_xy(x, y))
        copy.start()
        second_copies.append(copy)
    for copy in second_copies:
        copy.wait_recv()
    part = part + jnp.sum(ar2[...], axis=0)
    left = lanes((1, 128)) < 64
    total_n = jnp.sum(jnp.where(left, part, 0.0), axis=1, keepdims=True)
    total_d = jnp.sum(jnp.where(left, 0.0, part), axis=1, keepdims=True)
    alpha_ref[...] = total_n / total_d
    for copy in out_copies:
        copy.wait()
    for copy in rhs_copies + field_copies + coarse_copies + first_copies + second_copies:
        copy.wait_send()


def solution(mesh):
    ngz, ngy = mesh.shape["gz"], mesh.shape["gy"]
    nz = ngz // (NX_CHIPS * CORES)
    coarse = 4 * ngy - 1
    one = nz * CORES - 1
    two = NX_CHIPS * ngy - 1

    def body(right_side):
        out = jax.ShapeDtypeStruct(right_side.shape, F32)
        vm = pltpu.VMEM
        dma = pltpu.SemaphoreType.DMA
        precond, image, alpha = pl.pallas_call(
            functools.partial(kernel, ngz, ngy),
            name="cg_iteration",
            out_shape=(pltpu.VMEM(right_side.shape, F32), pltpu.VMEM(right_side.shape, F32), jax.ShapeDtypeStruct((1, 1), F32)),
            in_specs=[pl.BlockSpec(memory_space=pltpu.HBM)],
            out_specs=(
                pl.BlockSpec(memory_space=pl.ANY),
                pl.BlockSpec(memory_space=pl.ANY),
                pl.BlockSpec(memory_space=pltpu.VMEM),
            ),
            scratch_shapes=[
                vm((8, 8, 256), F32),
                vm((2, 64, 128), F32),
                vm((3, 2, 128, 128), F32),
                vm((2, 2, 2, 12, 8, 128), F32),
                vm((2, 2, 2 * ngy, 8, 128), F32),
                vm((2, ngy, 8, 128), F32),
                vm((2, 2, 2, 12, 8, 128), F32),
                vm((2, 2, 2, 12, 8, 128), F32),
                vm((2, 2, 2, 12, 8, 128), F32),
                vm((2, 12, 8, 128), F32),
                vm((2, 128, 128), F32),
                vm((3, 2, 128, 128), F32),
                vm((32, 128), F32),
                vm((ngy, 64, 128), F32),
                vm((2, 2, 2 * ngy, 8, 128), F32),
                vm((2, 2, 2 * ngy + 2, 8, 128), F32),
                vm((2, 2, 2 * ngy + 2, 8, 128), F32),
                vm((2, ngy, 8, 128), F32),
                vm((2, ngy + 2, 8, 128), F32),
                vm((4, 16, 128), F32),
                vm((2, 2, 128, 128), F32),
                vm((8, 8, 256), F32),
                vm((8, 8, 256), F32),
                vm((2, 1, 128), F32),
                vm((one, 1, 128), F32),
                vm((two, 1, 128), F32),
                pltpu.SemaphoreType.REGULAR, pltpu.SemaphoreType.REGULAR((2,)), pltpu.SemaphoreType.REGULAR,
                dma((3,)), dma((8,)), dma((8,)), dma((8,)), dma((8,)), dma((coarse,)), dma((coarse,)),
                dma((one,)), dma((one,)), dma((two,)), dma((two,)),
            ],
            compiler_params=pltpu.CompilerParams(collective_id=0, has_side_effects=True, vmem_limit_bytes=60000000),
        )(right_side)
        return alpha[:, :, None] * precond, right_side - alpha[:, :, None] * image

    return jax.shard_map(
        body,
        mesh=mesh,
        in_specs=(P("gz", "gy", None),),
        out_specs=(P("gz", "gy", None), P("gz", "gy", None)),
        check_vma=False,
    )
```
